32 devices in a mesh: grp: 2 (over y), var: 8 (over z, x), smp: 2 (over core).
Axes of the slice: x: 2, y: 2, z: 4, core: 2. Of those that a mesh axis runs over, the one named last changes fastest.
Arguments:
- genotypes: bfloat16 [15360, 1024], P(('grp', 'smp'), 'var'), parts along dimension 0, may hold values from 0 to 2, as said below
- ancestry_counts: int32 [15360, 32], P(('grp', 'smp')), parts along dimension 0, may hold values from 1 to 100
- residuals: int32 [15360, 16], P(('grp', 'smp')), parts along dimension 0, may hold values from -3000 to 3000
- freqs: float32 [64, 1024], P('grp', 'var'), parts along dimension 0, may hold values from 0.05 to 0.95
Outputs:
- q_new: float32 [15360, 32], P(('grp', 'smp', 'var')), parts along dimension 0
- q_gradient: float32 [15360, 32], P(('grp', 'smp', 'var')), parts along dimension 0
- p_new: float32 [64, 1024], P('grp', 'var'), parts along dimension 0
- p_gradient: float32 [64, 1024], P('grp', 'var'), parts along dimension 0
- z_score: float32 [64, 16, 1024], P('grp', None, 'var'), parts along dimension 0
The draws below stay inside these ranges and needn't reach their ends.
There are 2 independent parts, one for each index of `grp`. The reference program is written for one: setup_inputs(seed, part) draws one part's arguments, and reference() takes and returns one part's arrays. A program takes and returns all parts, laid end to end along the dimension named above; each array names one. Nothing has to cross between parts.
Inputs may be any that keep to these rules, and one draw needn't show every extreme that they name: `genotypes`: dosages lie in the closed range from 0 to 2.
All inputs are finite; a program needn't handle non-finite values.
Results may differ from the reference program's by a relative error of at most 0.0003.
Values sent between devices are 32-bit elements; how exact they have to be, the bound alone decides.
A program may use at most 64 MiB of HBM per device.

```python
import math
import jax
import jax.numpy as jnp
from jax import lax

ANC = 32
TRAITS = 16
MV = 128
SAMPLES = 7680
VARIANTS = 1024
N_VAR = 8


def draw_genotypes(key, part):
    logits = jax.random.uniform(jax.random.fold_in(key, 11), (1, VARIANTS), jnp.float32, -2.5, 2.5)
    block_rows = 960
    block_ids = jnp.arange(SAMPLES // block_rows, dtype=jnp.int32)

    def one_block(block_index):
        block_key = jax.random.fold_in(jax.random.fold_in(key, 12), block_index)
        first_key, second_key = jax.random.split(block_key)
        noise_one = 2.0 * jax.random.normal(first_key, (block_rows, VARIANTS), jnp.float32)
        noise_two = 2.0 * jax.random.normal(second_key, (block_rows, VARIANTS), jnp.float32)
        dosage = jax.nn.sigmoid(logits + noise_one) + jax.nn.sigmoid(logits + noise_two)
        return dosage
    blocks = lax.map(one_block, block_ids)
    return blocks.reshape(SAMPLES, VARIANTS).astype(jnp.bfloat16)


def with_ends(array, key, low, largest):
    longest = array.shape.index(max(array.shape))
    spots = []
    for shift in (0, 1):
        where = [jax.random.randint(jax.random.fold_in(key, axis), (), 0, length) for axis, length in enumerate(array.shape)]
        where[longest] = (where[longest] + shift) % array.shape[longest]
        spots.append(tuple(where))
    return array.at[spots[0]].set(low).at[spots[1]].set(largest)


def levels(own_key, dims, pieces, least, top_value):
    gain = 1.0
    for axis_at, shards_of in pieces:
        steps = jax.random.uniform(jax.random.fold_in(jax.random.fold_in(own_key, 6), axis_at), (shards_of,), jnp.float32, least / len(pieces), top_value / len(pieces))
        gain = gain * jnp.repeat(jnp.exp(steps), dims[axis_at] // shards_of).reshape((-1,) + (1,) * (len(dims) - 1 - axis_at))
    return gain


def setup_inputs(seed: int = 0, part: int = 0) -> dict:
    splits = jax.random.split(jax.random.key(seed), 5)
    own_keys = jax.random.split(jax.random.fold_in(splits[4], part), 5)
    return {
        "genotypes": draw_genotypes(jax.random.fold_in(jax.random.fold_in(splits[4], part), 71), part),
        "ancestry_counts": with_ends(jax.random.randint(own_keys[1], (SAMPLES, ANC), 1, 101), jax.random.fold_in(own_keys[1], 1), 1, 100).astype(jnp.int32),
        "residuals": with_ends(jax.random.randint(own_keys[2], (SAMPLES, TRAITS), -3000, 3001), jax.random.fold_in(own_keys[2], 1), -3000, 3000).astype(jnp.int32),
        "freqs": jnp.clip(0.05 + 0.9 * jax.random.uniform(own_keys[3], (ANC, VARIANTS), jnp.float32) ** levels(own_keys[3], (ANC, VARIANTS), ((1, 8),), -0.2, 0.2), 0.05, 0.95),
    }


def reference(genotypes, ancestry_counts, residuals, freqs):
    highest = lax.Precision.HIGHEST
    counts = ancestry_counts.astype(jnp.float32)
    fractions = counts / lax.optimization_barrier(jnp.sum(counts, axis=1, keepdims=True))
    residual = residuals.astype(jnp.float32) / 1000.0
    column_ids = jnp.arange(N_VAR, dtype=jnp.int32)

    def first_pass(state_pair, column):
        gradient, second = state_pair
        start = (column * MV).astype(jnp.int32)
        dosage = lax.dynamic_slice_in_dim(genotypes, start, MV, 1).astype(jnp.float32)
        freq_block = lax.dynamic_slice_in_dim(freqs, start, MV, 1)
        recon_block = jnp.dot(fractions, freq_block, precision=highest)
        ratio_a = dosage / recon_block
        ratio_b = (2.0 - dosage) / (1.0 - recon_block)
        excess = ratio_a - ratio_b
        gradient = gradient + jnp.dot(excess, freq_block.T, precision=highest)
        second = second + lax.optimization_barrier(jnp.sum(ratio_b, axis=1))
        excess_block = jnp.dot(fractions.T, excess, precision=highest)
        second_block = jnp.dot(fractions.T, ratio_b, precision=highest)
        return ((gradient, second), (excess_block, second_block))
    start_pair = (jnp.zeros((SAMPLES, ANC), jnp.float32), jnp.zeros((SAMPLES,), jnp.float32))
    (gradient, second), (excess_blocks, second_blocks) = lax.scan(first_pass, start_pair, column_ids)
    excess_sum = excess_blocks.transpose(1, 0, 2).reshape(ANC, VARIANTS)
    second_sum = second_blocks.transpose(1, 0, 2).reshape(ANC, VARIANTS)
    q_gradient = gradient / math.sqrt(VARIANTS)
    weighted = fractions * (gradient + second[:, None])
    q_new = weighted / lax.optimization_barrier(jnp.sum(weighted, axis=1, keepdims=True))
    allele_sum = excess_sum + second_sum
    p_new = freqs * allele_sum / (freqs * allele_sum + (1.0 - freqs) * second_sum)
    p_gradient = excess_sum * ANC / math.sqrt(SAMPLES)
    trait_rows = (q_new[:, :, None] * residual[:, None, :]).reshape(SAMPLES, ANC * TRAITS)
    squares = q_new * q_new

    def second_pass(state_pair, column):
        start = (column * MV).astype(jnp.int32)
        dosage = lax.dynamic_slice_in_dim(genotypes, start, MV, 1).astype(jnp.float32)
        freq_block = lax.dynamic_slice_in_dim(freqs, start, MV, 1)
        ratio_next = dosage / jnp.dot(q_new, freq_block, precision=highest)
        score_block = jnp.dot(trait_rows.T, ratio_next, precision=highest)
        info_block = jnp.dot(squares.T, ratio_next * ratio_next, precision=highest)
        return (state_pair, (score_block, info_block))
    _, (score_blocks, info_blocks) = lax.scan(second_pass, jnp.zeros((), jnp.float32), column_ids)
    score = score_blocks.transpose(1, 0, 2).reshape(ANC, TRAITS, VARIANTS)
    information = info_blocks.transpose(1, 0, 2).reshape(ANC, VARIANTS)
    z_score = score / jnp.sqrt(information + 1e-06)[:, None, :]
    return (q_new, q_gradient, p_new, p_gradient, z_score)
```

```python
import functools
import math

import jax
import jax.numpy as jnp
from jax import lax
from jax.experimental import pallas as pl
from jax.experimental.pallas import tpu as pltpu
from jax.sharding import PartitionSpec as P

MESH = pl.DeviceIdType.MESH
F32 = jnp.float32
BF16 = jnp.bfloat16
LIMIT = 67043328 - 491520
MOST = 5
LAG = 3


def normalize(fractions, gradient, second):
    weighted = fractions * (gradient + second[:, None])
    return weighted / jnp.sum(weighted, axis=1, keepdims=True)


def update_freqs(freqs, excess_sum, second_sum, sample_count):
    allele_sum = excess_sum + second_sum
    freq_next = freqs * allele_sum / (freqs * allele_sum + (1.0 - freqs) * second_sum)
    freq_gradient = excess_sum * freqs.shape[0] / math.sqrt(sample_count)
    return (freq_next, freq_gradient)


def shards_plain(genotypes, ancestry_counts, residuals, freqs):
    highest = lax.Precision.HIGHEST
    var_count = lax.axis_size("var")
    sample_rows = genotypes.shape[0]
    sample_count = sample_rows * lax.axis_size("smp")
    variant_count = genotypes.shape[1] * var_count
    anc_count = freqs.shape[0]
    trait_count = residuals.shape[1]
    counts = ancestry_counts.astype(jnp.float32)
    fractions = counts / jnp.sum(counts, axis=1, keepdims=True)
    dosage = genotypes.astype(jnp.float32)
    recon_rows = jnp.dot(fractions, freqs, precision=highest)
    ratio_a = dosage / recon_rows
    ratio_b = (2.0 - dosage) / (1.0 - recon_rows)
    excess = ratio_a - ratio_b
    gradient_part = jnp.dot(excess, freqs.T, precision=highest)
    second_part = jnp.sum(ratio_b, axis=1)
    excess_part = jnp.dot(fractions.T, excess, precision=highest)
    return_part = jnp.dot(fractions.T, ratio_b, precision=highest)
    share_rows = sample_rows // var_count
    first_row = lax.axis_index("var") * share_rows
    excess_sum, second_sum = lax.psum((excess_part, return_part), "smp")
    freq_next, freq_gradient = update_freqs(freqs, excess_sum, second_sum, sample_count)
    gradient_all, second_all = lax.psum((gradient_part, second_part), "var")
    fraction_next = normalize(fractions, gradient_all, second_all)
    own_next = lax.dynamic_slice_in_dim(fraction_next, first_row, share_rows, 0)
    own_gradient = lax.dynamic_slice_in_dim(gradient_all, first_row, share_rows, 0)
    scaled_gradient = own_gradient / math.sqrt(variant_count)
    ratio_next = dosage / jnp.dot(fraction_next, freqs, precision=highest)
    residual = residuals.astype(jnp.float32) / 1000.0
    trait_rows = (fraction_next[:, :, None] * residual[:, None, :]).reshape(
        sample_rows, anc_count * trait_count
    )
    score_part = jnp.dot(trait_rows.T, ratio_next, precision=highest)
    info_part = jnp.dot(
        (fraction_next * fraction_next).T, ratio_next * ratio_next, precision=highest
    )
    score_sum, info_sum = lax.psum((score_part, info_part), "smp")
    score_tiles = score_sum.reshape(anc_count, trait_count, genotypes.shape[1])
    z_score = score_tiles / jnp.sqrt(info_sum + 1e-06)[:, None, :]
    return (own_next, scaled_gradient, freq_next, freq_gradient, z_score)


def split(x):
    high = x.astype(BF16)
    return high, (x - high.astype(F32)).astype(BF16)


def dot(a, b):
    return jnp.dot(a, b, preferred_element_type=F32)


def dot_lanes(a, b):
    return lax.dot_general(a, b, (((1,), (1,)), ((), ())), preferred_element_type=F32)


def kernel(
    dims,
    geno_in, counts_in, resid_in, freqs_in,
    q_out, g_out, p_out, pg_out, z_out,
    geno, counts, resid, freqs, dos, qf, gf, fcol, frow, ebuf, tbuf,
    acc_ex, acc_sc, acc_in,
    xs, xr, zs, er, mr, go, gp, fs, fr, ss, sr,
    xs_s, xs_r, e_s, e_r, m_s, m_r, o_s, o_r, xa_s, xa_r, f_s, f_r, s_s, s_r, in_s,
):
    chunks, width, half, variant_count, sample_count, share, var_n = dims
    sub = width // 128
    anc = freqs.shape[0]
    traits = resid.shape[0]
    mv = freqs.shape[1]
    me = lax.axis_index("var")
    core = lax.axis_index("smp")
    x = lax.rem(me, 2)
    z = me // 2
    zn = z + 1 - 2 * lax.rem(z, 2)
    middle = jnp.logical_or(z == 1, z == 2)
    end = jnp.logical_or(z == 0, z == 3)
    partner = {"var": z * 2 + (1 - x)}
    twin = {"smp": 1 - core}
    beside = {"var": zn * 2 + x}
    across = {"var": lax.rem(7 - z, 4) * 2 + x}

    def load(src, dst, which, base=None, size=None):
        if base is not None:
            src, dst = src.at[pl.ds(base, size), :], dst.at[pl.ds(base, size), :]
        return pltpu.make_async_copy(src, dst, in_s.at[which])

    def load_lanes(src, dst, which, base, size):
        return pltpu.make_async_copy(
            src.at[:, pl.ds(base, size)], dst.at[:, pl.ds(base, size)], in_s.at[which]
        )

    far_half = pl.multiple_of((1 - x) * half, 128)
    near_half = pl.multiple_of(x * half, 128)
    freqs_load = load(freqs_in, freqs, 0)
    first_loads = (
        load_lanes(counts_in, counts, 1, far_half, width),
        load(geno_in, geno, 2, far_half, width),
    )
    later_loads = ()
    if chunks > 1:
        far_next = pl.multiple_of(far_half + width, 128)
        later_loads = (
            load_lanes(counts_in, counts, 3, far_next, half - width),
            load(geno_in, geno, 4, far_next, half - width),
        )
    near_loads = (
        load_lanes(counts_in, counts, 5, near_half, half),
        load(geno_in, geno, 6, near_half, half),
    )
    resid_load = load(resid_in, resid, 7)
    for item in (freqs_load,) + first_loads + later_loads + near_loads + (resid_load,):
        item.start()

    barrier = pltpu.get_barrier_semaphore()
    for peer in (partner, twin, beside):
        pl.semaphore_signal(barrier, inc=1, device_id=peer, device_id_type=MESH)

    @pl.when(middle)
    def _():
        pl.semaphore_signal(barrier, inc=1, device_id=across, device_id_type=MESH)

    freqs_load.wait()
    p = freqs[...]
    p_hi, p_lo = split(p)
    stack = jnp.concatenate([p_hi.astype(F32), p_lo.astype(F32)] * 2, axis=0)
    fcol[...] = stack.T.astype(BF16)
    frow[0:anc, 0:mv] = p_hi
    frow[0:anc, mv:] = p_hi
    frow[anc:, 0:mv] = p_lo
    frow[anc:, mv:] = p_lo
    acc_ex[...] = jnp.zeros_like(acc_ex)
    acc_sc[...] = jnp.zeros_like(acc_sc)
    acc_in[...] = jnp.zeros_like(acc_in)

    def lanes(which, c):
        return pl.multiple_of(which * half + c * width, 128)

    def first_pass(off):
        d = geno[pl.ds(off, width), :].astype(F32).T
        dos[:, pl.ds(off, width)] = d.astype(BF16)
        c = counts[:, pl.ds(off, width)].astype(F32)
        total = jnp.sum(c, axis=0, keepdims=True)
        cb = c.astype(BF16)
        none = jnp.zeros_like(cb)
        u = dot(fcol[...], jnp.concatenate([cb, cb, none, none], axis=0))
        w = total - u
        inverse = 1.0 / (u * w)
        b = (2.0 - d) * u * inverse
        e = d * w * inverse - b
        e_hi, e_lo = split(e)
        b_hi, b_lo = split(b)
        ebuf[0:mv, :] = e_hi
        ebuf[mv : 2 * mv, :] = e_lo
        ebuf[2 * mv : 3 * mv, :] = b_hi
        ebuf[3 * mv :, :] = b_lo
        g = dot(frow[...], ebuf[0 : 2 * mv, :])
        acc_ex[...] += dot_lanes(ebuf[...], jnp.concatenate([cb] * (128 // anc), axis=0))
        return (g[0:anc, :] + g[anc:, :]) * total

    def second_pass(off, g):
        c = counts[:, pl.ds(off, width)].astype(F32)
        f = c / jnp.sum(c, axis=0, keepdims=True)
        second = 2.0 * variant_count - jnp.sum(f * g, axis=0, keepdims=True)
        weighted = f * (g + second)
        q = weighted / jnp.sum(weighted, axis=0, keepdims=True)
        qf[:, pl.ds(off, width)] = q
        gf[:, pl.ds(off, width)] = g * (1.0 / math.sqrt(variant_count))
        q_hi, q_lo = split(q)
        recon = dot(fcol[...], jnp.concatenate([q_hi, q_hi, q_lo, q_lo], axis=0))
        r = dos[:, pl.ds(off, width)].astype(F32) / recon
        r_hi, r_lo = split(r)
        s_hi, s_lo = split(r * r)
        t = resid[:, pl.ds(off, width)].astype(F32)
        for k in range(anc):
            t_hi, t_lo = split(q[k : k + 1, :] * t)
            tbuf[traits * k : traits * (k + 1), 0:width] = t_hi
            tbuf[traits * k : traits * (k + 1), width:] = t_lo
        r_cat = jnp.concatenate([r_hi, r_lo], axis=0)
        acc_sc[...] += dot_lanes(tbuf[...], jnp.concatenate([r_cat, r_cat], axis=1))
        y_hi, y_lo = split(q * q)
        none = jnp.zeros_like(y_hi)
        acc_in[...] += dot_lanes(
            jnp.concatenate([s_hi, s_lo], axis=0),
            jnp.concatenate([y_hi, y_lo, none, none], axis=0),
        )

    def copy(src, dst, send, recv, peer):
        return pltpu.make_async_remote_copy(
            src_ref=src, dst_ref=dst, send_sem=send, recv_sem=recv, device_id=peer, device_id_type=MESH
        )

    def x_reduce(t):
        return copy(xs.at[t], xr.at[t], xs_s.at[t], xs_r.at[t], partner)

    def inward(t):
        return copy(zs.at[t], er.at[t], e_s.at[t], e_r.at[t], beside)

    def exchange(t):
        return copy(zs.at[t], mr.at[t], m_s.at[t], m_r.at[t], across)

    def outward(t):
        return copy(go.at[t], go.at[t], o_s.at[t], o_r.at[t], beside)

    def x_gather(t):
        return copy(go.at[t], gp.at[t], xa_s.at[t], xa_r.at[t], partner)

    def put(ref, c, g):
        for j in range(sub):
            ref[c * sub + j] = g[:, 128 * j : 128 * (j + 1)]

    def take(ref, c):
        return jnp.concatenate([ref[c * sub + j] for j in range(sub)], axis=1)

    for item in first_loads:
        item.wait()
    put(xs, 0, first_pass(lanes(1 - x, 0)))

    @pl.when(middle)
    def _():
        pl.semaphore_wait(barrier, 4)

    @pl.when(end)
    def _():
        pl.semaphore_wait(barrier, 3)

    for j in range(sub):
        x_reduce(j).start()
    for item in later_loads:
        item.wait()

    def step_far(c, carry):
        put(xs, c, first_pass(lanes(1 - x, c)))
        for j in range(sub):
            x_reduce(c * sub + j).start()
        return carry

    lax.fori_loop(1, chunks, step_far, 0)
    for item in near_loads:
        item.wait()

    def add_inward(t):
        inward(t).wait_recv()
        zs[t] = zs[t] + er[t]
        exchange(t).start()

    def add_exchange(t):
        exchange(t).wait_recv()
        go[t] = zs[t] + mr[t]
        outward(t).start()
        x_gather(t).start()

    def step_near(c, carry):
        put(zs, c, first_pass(lanes(x, c)))
        for j in range(sub):
            t = c * sub + j
            x_reduce(t).wait_recv()
            zs[t] = zs[t] + xr[t]

            @pl.when(end)
            def _(t=t):
                inward(t).start()

            @pl.when(jnp.logical_and(middle, c >= LAG))
            def _(t=t):
                add_inward(t - LAG * sub)

        return carry

    lax.fori_loop(0, chunks, step_near, 0)

    ex = acc_ex[0:mv, :] + acc_ex[mv : 2 * mv, :]
    re = acc_ex[2 * mv : 3 * mv, :] + acc_ex[3 * mv :, :]
    fs[0:anc, :] = ex.T[0:anc, :]
    fs[anc:, :] = re.T[0:anc, :]
    freq_copy = copy(fs, fr, f_s, f_r, twin)
    freq_copy.start()

    @pl.when(middle)
    def _():
        def step_inward(t, carry):
            add_inward(t)
            return carry

        lax.fori_loop(max(0, chunks - LAG) * sub, min(LAG, chunks) * sub, step_inward, 0)

    resid_load.wait()

    def step_own(c, carry):
        for j in range(sub):
            t = c * sub + j

            @pl.when(jnp.logical_and(middle, c + LAG < chunks))
            def _(t=t):
                add_inward(t + LAG * sub)

            @pl.when(middle)
            def _(t=t):
                add_exchange(t)

            @pl.when(end)
            def _(t=t):
                outward(t).wait_recv()
                x_gather(t).start()

        second_pass(lanes(x, c), take(go, c))
        return carry

    lax.fori_loop(0, chunks, step_own, 0)

    def step_other(c, carry):
        for j in range(sub):
            x_gather(c * sub + j).wait_recv()
        second_pass(lanes(1 - x, c), take(gp, c))
        return carry

    lax.fori_loop(0, chunks, step_other, 0)

    tiles = anc * traits
    ss[0:tiles, :] = acc_sc[:, 0:mv] + acc_sc[:, mv:]
    info = (acc_in[0:mv, :] + acc_in[mv:, :]).T
    ss[tiles:, :] = info[0:anc, :] + info[anc : 2 * anc, :]
    score_copy = copy(ss, sr, s_s, s_r, twin)
    score_copy.start()

    freq_copy.wait_recv()
    sums = fs[...] + fr[...]
    excess_sum = sums[0:anc, :]
    second_sum = sums[anc:, :]
    freq_next, freq_gradient = update_freqs(freqs[...], excess_sum, second_sum, sample_count)
    p_out[...] = freq_next
    pg_out[...] = freq_gradient

    for v in range(var_n):

        @pl.when(me == v)
        def _():
            q_out[...] = qf[:, share * v : share * (v + 1)]
            g_out[...] = gf[:, share * v : share * (v + 1)]

    def drain(t, carry):
        x_reduce(t).wait_send()
        x_gather(t).wait_send()

        @pl.when(end)
        def _():
            inward(t).wait_send()

        @pl.when(middle)
        def _():
            exchange(t).wait_send()
            outward(t).wait_send()

        return carry

    lax.fori_loop(0, chunks * sub, drain, 0)
    freq_copy.wait_send()
    score_copy.wait_recv()
    info_sum = ss[tiles:, :] + sr[tiles:, :]
    scale = 0.001 / jnp.sqrt(info_sum + 1e-06)
    for k in range(anc):
        at = slice(traits * k, traits * (k + 1))
        z_out[at, :] = (ss[at, :] + sr[at, :]) * scale[k : k + 1, :]
    score_copy.wait_send()


def store_kernel(*refs):
    count = len(refs) // 2
    sems = refs[-1]
    copies = [pltpu.make_async_copy(refs[i], refs[count + i], sems.at[i]) for i in range(count)]
    for item in copies:
        item.start()
    for item in copies:
        item.wait()


def store(*arrays):
    return pl.pallas_call(
        store_kernel,
        out_shape=tuple(jax.ShapeDtypeStruct(a.shape, a.dtype) for a in arrays),
        in_specs=[pl.BlockSpec(memory_space=pltpu.VMEM)] * len(arrays),
        out_specs=(pl.BlockSpec(memory_space=pl.ANY),) * len(arrays),
        scratch_shapes=[pltpu.SemaphoreType.DMA((len(arrays),))],
        compiler_params=pltpu.CompilerParams(vmem_limit_bytes=1024 * 1024),
        name="store",
    )(*arrays)


def fits(genotypes, residuals, freqs, var_n):
    samples, mv = genotypes.shape
    anc = freqs.shape[0]
    return (
        var_n == 8
        and lax.axis_size("smp") == 2
        and anc == 32
        and mv == 128
        and residuals.shape[1] % 16 == 0
        and samples % (2 * 128) == 0
        and samples % var_n == 0
    )


def shards(genotypes, ancestry_counts, residuals, freqs):
    var_n = lax.axis_size("var")
    if not fits(genotypes, residuals, freqs, var_n):
        return shards_plain(genotypes, ancestry_counts, residuals, freqs)
    samples, mv = genotypes.shape
    anc = freqs.shape[0]
    traits = residuals.shape[1]
    half = samples // 2
    tiles = half // 128
    chunks = max(n for n in range(1, MOST + 1) if tiles % n == 0)
    width = half // chunks
    share = samples // var_n
    dims = (chunks, width, half, mv * var_n, samples * lax.axis_size("smp"), share, var_n)
    vmem = pl.BlockSpec(memory_space=pltpu.VMEM)
    dma = pltpu.SemaphoreType.DMA
    part = pltpu.VMEM((half // 128, anc, 128), F32)
    flags = dma((half // 128,))
    results = pl.pallas_call(
        functools.partial(kernel, dims),
        out_shape=(
            pltpu.VMEM((anc, share), F32),
            pltpu.VMEM((anc, share), F32),
            pltpu.VMEM((anc, mv), F32),
            pltpu.VMEM((anc, mv), F32),
            pltpu.VMEM((anc * traits, mv), F32),
        ),
        in_specs=[pl.BlockSpec(memory_space=pltpu.HBM)] * 4,
        out_specs=(vmem,) * 5,
        scratch_shapes=[
            pltpu.VMEM((samples, mv), BF16),
            pltpu.VMEM((anc, samples), jnp.int32),
            pltpu.VMEM((traits, samples), jnp.int32),
            pltpu.VMEM((anc, mv), F32),
            pltpu.VMEM((mv, samples), BF16),
            pltpu.VMEM((anc, samples), F32),
            pltpu.VMEM((anc, samples), F32),
            pltpu.VMEM((mv, 4 * anc), BF16),
            pltpu.VMEM((2 * anc, 2 * mv), BF16),
            pltpu.VMEM((4 * mv, width), BF16),
            pltpu.VMEM((anc * traits, 2 * width), BF16),
            pltpu.VMEM((4 * mv, 128), F32),
            pltpu.VMEM((anc * traits, 2 * mv), F32),
            pltpu.VMEM((2 * mv, 128), F32),
            part, part, part, part, part, part, part,
            pltpu.VMEM((2 * anc, mv), F32),
            pltpu.VMEM((2 * anc, mv), F32),
            pltpu.VMEM((anc * traits + anc, mv), F32),
            pltpu.VMEM((anc * traits + anc, mv), F32),
            flags, flags, flags, flags, flags, flags, flags, flags, flags, flags,
            dma, dma, dma, dma, dma((8,)),
        ],
        compiler_params=pltpu.CompilerParams(collective_id=0, has_side_effects=True, vmem_limit_bytes=LIMIT),
        name="em_step",
    )(genotypes, ancestry_counts.T, residuals.T, freqs)
    q_t, g_t, p_new, p_grad, z_flat = store(*results)
    return (q_t.T, g_t.T, p_new, p_grad, z_flat.reshape(anc, traits, mv))


def solution(mesh):
    in_specs = (
        P(("grp", "smp"), "var"),
        P(("grp", "smp"), None),
        P(("grp", "smp"), None),
        P("grp", "var"),
    )
    out_specs = (
        P(("grp", "smp", "var"), None),
        P(("grp", "smp", "var"), None),
        P("grp", "var"),
        P("grp", "var"),
        P("grp", None, "var"),
    )
    return jax.shard_map(shards, mesh=mesh, in_specs=in_specs, out_specs=out_specs, check_vma=False)
```

```python
import functools
import math

import jax
import jax.numpy as jnp
from jax import lax
from jax.experimental import pallas as pl
from jax.experimental.pallas import tpu as pltpu
from jax.sharding import PartitionSpec as P

MESH = pl.DeviceIdType.MESH
F32 = jnp.float32
BF16 = jnp.bfloat16
LIMIT = 67043328 - 491520
MOST = 5
LAG = 3


def normalize(fractions, gradient, second):
    weighted = fractions * (gradient + second[:, None])
    return weighted / jnp.sum(weighted, axis=1, keepdims=True)


def update_freqs(freqs, excess_sum, second_sum, sample_count):
    allele_sum = excess_sum + second_sum
    freq_next = freqs * allele_sum / (freqs * allele_sum + (1.0 - freqs) * second_sum)
    freq_gradient = excess_sum * freqs.shape[0] / math.sqrt(sample_count)
    return (freq_next, freq_gradient)


def shards_plain(genotypes, ancestry_counts, residuals, freqs):
    highest = lax.Precision.HIGHEST
    var_count = lax.axis_size("var")
    sample_rows = genotypes.shape[0]
    sample_count = sample_rows * lax.axis_size("smp")
    variant_count = genotypes.shape[1] * var_count
    anc_count = freqs.shape[0]
    trait_count = residuals.shape[1]
    counts = ancestry_counts.astype(jnp.float32)
    fractions = counts / jnp.sum(counts, axis=1, keepdims=True)
    dosage = genotypes.astype(jnp.float32)
    recon_rows = jnp.dot(fractions, freqs, precision=highest)
    ratio_a = dosage / recon_rows
    ratio_b = (2.0 - dosage) / (1.0 - recon_rows)
    excess = ratio_a - ratio_b
    gradient_part = jnp.dot(excess, freqs.T, precision=highest)
    second_part = jnp.sum(ratio_b, axis=1)
    excess_part = jnp.dot(fractions.T, excess, precision=highest)
    return_part = jnp.dot(fractions.T, ratio_b, precision=highest)
    share_rows = sample_rows // var_count
    first_row = lax.axis_index("var") * share_rows
    excess_sum, second_sum = lax.psum((excess_part, return_part), "smp")
    freq_next, freq_gradient = update_freqs(freqs, excess_sum, second_sum, sample_count)
    gradient_all, second_all = lax.psum((gradient_part, second_part), "var")
    fraction_next = normalize(fractions, gradient_all, second_all)
    own_next = lax.dynamic_slice_in_dim(fraction_next, first_row, share_rows, 0)
    own_gradient = lax.dynamic_slice_in_dim(gradient_all, first_row, share_rows, 0)
    scaled_gradient = own_gradient / math.sqrt(variant_count)
    ratio_next = dosage / jnp.dot(fraction_next, freqs, precision=highest)
    residual = residuals.astype(jnp.float32) / 1000.0
    trait_rows = (fraction_next[:, :, None] * residual[:, None, :]).reshape(
        sample_rows, anc_count * trait_count
    )
    score_part = jnp.dot(trait_rows.T, ratio_next, precision=highest)
    info_part = jnp.dot(
        (fraction_next * fraction_next).T, ratio_next * ratio_next, precision=highest
    )
    score_sum, info_sum = lax.psum((score_part, info_part), "smp")
    score_tiles = score_sum.reshape(anc_count, trait_count, genotypes.shape[1])
    z_score = score_tiles / jnp.sqrt(info_sum + 1e-06)[:, None, :]
    return (own_next, scaled_gradient, freq_next, freq_gradient, z_score)


def split(x):
    high = x.astype(BF16)
    return high, (x - high.astype(F32)).astype(BF16)


def dot(a, b):
    return jnp.dot(a, b, preferred_element_type=F32)


def dot_lanes(a, b):
    return lax.dot_general(a, b, (((1,), (1,)), ((), ())), preferred_element_type=F32)


def kernel(
    dims,
    geno_in, counts_in, resid_in, freqs_in,
    q_out, g_out, p_out, pg_out, z_out,
    geno, counts, resid, freqs, dos, qf, gf, fcol, frow, ebuf, tbuf,
    acc_ex, acc_sc, acc_in,
    xs, xr, zs, er, mr, go, gp, fs, fr, ss, sr,
    xs_s, xs_r, z_s, z_r, m_s, m_r, xa_s, xa_r, f_s, f_r, s_s, s_r, in_s,
):
    chunks, width, half, variant_count, sample_count, share, var_n = dims
    sub = width // 128
    anc = freqs.shape[0]
    traits = resid.shape[0]
    mv = freqs.shape[1]
    me = lax.axis_index("var")
    core = lax.axis_index("smp")
    x = lax.rem(me, 2)
    z = me // 2
    zn = z + 1 - 2 * lax.rem(z, 2)
    middle = jnp.logical_or(z == 1, z == 2)
    end = jnp.logical_or(z == 0, z == 3)
    partner = {"var": z * 2 + (1 - x)}
    twin = {"smp": 1 - core}
    beside = {"var": zn * 2 + x}
    across = {"var": lax.rem(7 - z, 4) * 2 + x}

    def load(src, dst, which, base=None, size=None):
        if base is not None:
            src, dst = src.at[pl.ds(base, size), :], dst.at[pl.ds(base, size), :]
        return pltpu.make_async_copy(src, dst, in_s.at[which])

    def load_lanes(src, dst, which, base, size):
        return pltpu.make_async_copy(
            src.at[:, pl.ds(base, size)], dst.at[:, pl.ds(base, size)], in_s.at[which]
        )

    far_half = pl.multiple_of((1 - x) * half, 128)
    near_half = pl.multiple_of(x * half, 128)
    freqs_load = load(freqs_in, freqs, 0)
    first_loads = (
        load_lanes(counts_in, counts, 1, far_half, width),
        load(geno_in, geno, 2, far_half, width),
    )
    later_loads = ()
    if chunks > 1:
        far_next = pl.multiple_of(far_half + width, 128)
        later_loads = (
            load_lanes(counts_in, counts, 3, far_next, half - width),
            load(geno_in, geno, 4, far_next, half - width),
        )
    near_loads = (
        load_lanes(counts_in, counts, 5, near_half, half),
        load(geno_in, geno, 6, near_half, half),
    )
    resid_load = load(resid_in, resid, 7)
    for item in (freqs_load,) + first_loads + later_loads + near_loads + (resid_load,):
        item.start()

    barrier = pltpu.get_barrier_semaphore()
    for peer in (partner, twin, beside):
        pl.semaphore_signal(barrier, inc=1, device_id=peer, device_id_type=MESH)

    @pl.when(middle)
    def _():
        pl.semaphore_signal(barrier, inc=1, device_id=across, device_id_type=MESH)

    freqs_load.wait()
    p = freqs[...]
    p_hi, p_lo = split(p)
    stack = jnp.concatenate([p_hi.astype(F32), p_lo.astype(F32)] * 2, axis=0)
    fcol[...] = stack.T.astype(BF16)
    frow[0:anc, 0:mv] = p_hi
    frow[0:anc, mv:] = p_hi
    frow[anc:, 0:mv] = p_lo
    frow[anc:, mv:] = p_lo
    acc_ex[...] = jnp.zeros_like(acc_ex)
    acc_sc[...] = jnp.zeros_like(acc_sc)
    acc_in[...] = jnp.zeros_like(acc_in)

    def lanes(which, c):
        return pl.multiple_of(which * half + c * width, 128)

    def first_pass(off):
        d = geno[pl.ds(off, width), :].astype(F32).T
        dos[:, pl.ds(off, width)] = d.astype(BF16)
        c = counts[:, pl.ds(off, width)].astype(F32)
        total = jnp.sum(c, axis=0, keepdims=True)
        cb = c.astype(BF16)
        none = jnp.zeros_like(cb)
        u = dot(fcol[...], jnp.concatenate([cb, cb, none, none], axis=0))
        w = total - u
        inverse = 1.0 / (u * w)
        b = (2.0 - d) * u * inverse
        e = d * w * inverse - b
        e_hi, e_lo = split(e)
        b_hi, b_lo = split(b)
        ebuf[0:mv, :] = e_hi
        ebuf[mv : 2 * mv, :] = e_lo
        ebuf[2 * mv : 3 * mv, :] = b_hi
        ebuf[3 * mv :, :] = b_lo
        g = dot(frow[...], ebuf[0 : 2 * mv, :])
        acc_ex[...] += dot_lanes(ebuf[...], jnp.concatenate([cb] * (128 // anc), axis=0))
        return (g[0:anc, :] + g[anc:, :]) * total

    def second_pass(off, g):
        c = counts[:, pl.ds(off, width)].astype(F32)
        f = c / jnp.sum(c, axis=0, keepdims=True)
        second = 2.0 * variant_count - jnp.sum(f * g, axis=0, keepdims=True)
        weighted = f * (g + second)
        q = weighted / jnp.sum(weighted, axis=0, keepdims=True)
        qf[:, pl.ds(off, width)] = q
        gf[:, pl.ds(off, width)] = g * (1.0 / math.sqrt(variant_count))
        q_hi, q_lo = split(q)
        recon = dot(fcol[...], jnp.concatenate([q_hi, q_hi, q_lo, q_lo], axis=0))
        r = dos[:, pl.ds(off, width)].astype(F32) / recon
        r_hi, r_lo = split(r)
        s_hi, s_lo = split(r * r)
        t = resid[:, pl.ds(off, width)].astype(F32)
        r_cat = jnp.concatenate([r_hi, r_lo], axis=0)
        r_cat = jnp.concatenate([r_cat, r_cat], axis=1)
        step = anc // 2
        for m in range(2):
            for k in range(step * m, step * (m + 1)):
                t_hi, t_lo = split(q[k : k + 1, :] * t)
                tbuf[traits * k : traits * (k + 1), 0:width] = t_hi
                tbuf[traits * k : traits * (k + 1), width:] = t_lo
            at = slice(traits * step * m, traits * step * (m + 1))
            acc_sc[at, :] += dot_lanes(tbuf[at, :], r_cat)
        y_hi, y_lo = split(q * q)
        none = jnp.zeros_like(y_hi)
        acc_in[...] += dot_lanes(
            jnp.concatenate([y_hi, y_lo], axis=0), jnp.concatenate([s_hi, s_lo], axis=0)
        )

    def copy(src, dst, send, recv, peer):
        return pltpu.make_async_remote_copy(
            src_ref=src, dst_ref=dst, send_sem=send, recv_sem=recv, device_id=peer, device_id_type=MESH
        )

    def x_reduce(t):
        return copy(xs.at[t], xr.at[t], xs_s, xs_r.at[t], partner)

    def inward(t):
        return copy(zs.at[t], er.at[t], z_s, z_r.at[t], beside)

    def exchange(t):
        return copy(zs.at[t], mr.at[t], m_s, m_r.at[t], across)

    def outward(t):
        return copy(go.at[t], go.at[t], z_s, z_r.at[t], beside)

    def x_gather(c, j):
        return copy(go.at[c * sub + j], gp.at[c * sub + j], xa_s, xa_r.at[c], partner)

    def x_gathered(c):
        at = pl.ds(c * sub, sub)
        return copy(go.at[at], gp.at[at], xa_s, xa_r.at[c], partner)

    def put(ref, c, g):
        for j in range(sub):
            ref[c * sub + j] = g[:, 128 * j : 128 * (j + 1)]

    def take(ref, c):
        return jnp.concatenate([ref[c * sub + j] for j in range(sub)], axis=1)

    for item in first_loads:
        item.wait()
    put(xs, 0, first_pass(lanes(1 - x, 0)))

    @pl.when(middle)
    def _():
        pl.semaphore_wait(barrier, 4)

    @pl.when(end)
    def _():
        pl.semaphore_wait(barrier, 3)

    for j in range(sub):
        x_reduce(j).start()
    for item in later_loads:
        item.wait()

    def step_far(c, carry):
        put(xs, c, first_pass(lanes(1 - x, c)))
        for j in range(sub):
            x_reduce(c * sub + j).start()
        return carry

    lax.fori_loop(1, chunks, step_far, 0)
    for item in near_loads:
        item.wait()

    def add_inward(t):
        inward(t).wait_recv()
        zs[t] = zs[t] + er[t]
        exchange(t).start()

    def add_exchange(c, j):
        t = c * sub + j
        exchange(t).wait_recv()
        go[t] = zs[t] + mr[t]
        outward(t).start()
        x_gather(c, j).start()

    def step_near(c, carry):
        put(zs, c, first_pass(lanes(x, c)))
        for j in range(sub):
            t = c * sub + j
            x_reduce(t).wait_recv()
            zs[t] = zs[t] + xr[t]

            @pl.when(end)
            def _(t=t):
                inward(t).start()

            @pl.when(jnp.logical_and(middle, c >= LAG))
            def _(t=t):
                add_inward(t - LAG * sub)

        return carry

    lax.fori_loop(0, chunks, step_near, 0)

    ex = acc_ex[0:mv, :] + acc_ex[mv : 2 * mv, :]
    re = acc_ex[2 * mv : 3 * mv, :] + acc_ex[3 * mv :, :]
    fs[0:anc, :] = ex.T[0:anc, :]
    fs[anc:, :] = re.T[0:anc, :]
    freq_copy = copy(fs, fr, f_s, f_r, twin)
    freq_copy.start()

    @pl.when(middle)
    def _():
        def step_inward(t, carry):
            add_inward(t)
            return carry

        def step_exchange(c, carry):
            for j in range(sub):
                t = c * sub + j

                @pl.when(c + LAG < chunks)
                def _(t=t):
                    add_inward(t + LAG * sub)

                add_exchange(c, j)
            return carry

        lax.fori_loop(max(0, chunks - LAG) * sub, min(LAG, chunks) * sub, step_inward, 0)
        lax.fori_loop(0, chunks, step_exchange, 0)

    resid_load.wait()

    def step_own(c, carry):
        for j in range(sub):
            t = c * sub + j

            @pl.when(end)
            def _(t=t, j=j):
                outward(t).wait_recv()
                x_gather(c, j).start()

        second_pass(lanes(x, c), take(go, c))
        return carry

    lax.fori_loop(0, chunks, step_own, 0)

    def step_other(c, carry):
        x_gathered(c).wait_recv()
        second_pass(lanes(1 - x, c), take(gp, c))
        return carry

    lax.fori_loop(0, chunks, step_other, 0)

    tiles = anc * traits
    ss[0:tiles, :] = acc_sc[:, 0:mv] + acc_sc[:, mv:]
    info = acc_in[0:anc, :] + acc_in[anc:, :]
    ss[tiles:, :] = info[:, 0:mv] + info[:, mv:]
    score_copy = copy(ss, sr, s_s, s_r, twin)
    score_copy.start()

    freq_copy.wait_recv()
    sums = fs[...] + fr[...]
    excess_sum = sums[0:anc, :]
    second_sum = sums[anc:, :]
    freq_next, freq_gradient = update_freqs(freqs[...], excess_sum, second_sum, sample_count)
    p_out[...] = freq_next
    pg_out[...] = freq_gradient

    for v in range(var_n):

        @pl.when(me == v)
        def _():
            q_out[...] = qf[:, share * v : share * (v + 1)]
            g_out[...] = gf[:, share * v : share * (v + 1)]

    copy(xs, xr, xs_s, xs_r.at[0], partner).wait_send()
    copy(go, gp, xa_s, xa_r.at[0], partner).wait_send()
    copy(zs, er, z_s, z_r.at[0], beside).wait_send()

    @pl.when(middle)
    def _():
        copy(zs, mr, m_s, m_r.at[0], across).wait_send()

    freq_copy.wait_send()
    score_copy.wait_recv()
    info_sum = ss[tiles:, :] + sr[tiles:, :]
    scale = 0.001 / jnp.sqrt(info_sum + 1e-06)
    for k in range(anc):
        at = slice(traits * k, traits * (k + 1))
        z_out[at, :] = (ss[at, :] + sr[at, :]) * scale[k : k + 1, :]
    score_copy.wait_send()


def store_kernel(*refs):
    count = len(refs) // 2
    sems = refs[-1]
    copies = [pltpu.make_async_copy(refs[i], refs[count + i], sems.at[i]) for i in range(count)]
    for item in copies:
        item.start()
    for item in copies:
        item.wait()


def store(*arrays):
    return pl.pallas_call(
        store_kernel,
        out_shape=tuple(jax.ShapeDtypeStruct(a.shape, a.dtype) for a in arrays),
        in_specs=[pl.BlockSpec(memory_space=pltpu.VMEM)] * len(arrays),
        out_specs=(pl.BlockSpec(memory_space=pl.ANY),) * len(arrays),
        scratch_shapes=[pltpu.SemaphoreType.DMA((len(arrays),))],
        compiler_params=pltpu.CompilerParams(vmem_limit_bytes=1024 * 1024),
        name="store",
    )(*arrays)


def fits(genotypes, residuals, freqs, var_n):
    samples, mv = genotypes.shape
    anc = freqs.shape[0]
    return (
        var_n == 8
        and lax.axis_size("smp") == 2
        and anc == 32
        and mv == 128
        and residuals.shape[1] % 16 == 0
        and samples % (2 * 128) == 0
        and samples % var_n == 0
    )


def shards(genotypes, ancestry_counts, residuals, freqs):
    var_n = lax.axis_size("var")
    if not fits(genotypes, residuals, freqs, var_n):
        return shards_plain(genotypes, ancestry_counts, residuals, freqs)
    samples, mv = genotypes.shape
    anc = freqs.shape[0]
    traits = residuals.shape[1]
    half = samples // 2
    tiles = half // 128
    chunks = max(n for n in range(1, MOST + 1) if tiles % n == 0)
    width = half // chunks
    share = samples // var_n
    dims = (chunks, width, half, mv * var_n, samples * lax.axis_size("smp"), share, var_n)
    vmem = pl.BlockSpec(memory_space=pltpu.VMEM)
    dma = pltpu.SemaphoreType.DMA
    part = pltpu.VMEM((half // 128, anc, 128), F32)
    flags = dma((half // 128,))
    results = pl.pallas_call(
        functools.partial(kernel, dims),
        out_shape=(
            pltpu.VMEM((anc, share), F32),
            pltpu.VMEM((anc, share), F32),
            pltpu.VMEM((anc, mv), F32),
            pltpu.VMEM((anc, mv), F32),
            pltpu.VMEM((anc * traits, mv), F32),
        ),
        in_specs=[pl.BlockSpec(memory_space=pltpu.HBM)] * 4,
        out_specs=(vmem,) * 5,
        scratch_shapes=[
            pltpu.VMEM((samples, mv), BF16),
            pltpu.VMEM((anc, samples), jnp.int32),
            pltpu.VMEM((traits, samples), jnp.int32),
            pltpu.VMEM((anc, mv), F32),
            pltpu.VMEM((mv, samples), BF16),
            pltpu.VMEM((anc, samples), F32),
            pltpu.VMEM((anc, samples), F32),
            pltpu.VMEM((mv, 4 * anc), BF16),
            pltpu.VMEM((2 * anc, 2 * mv), BF16),
            pltpu.VMEM((4 * mv, width), BF16),
            pltpu.VMEM((anc * traits, 2 * width), BF16),
            pltpu.VMEM((4 * mv, 128), F32),
            pltpu.VMEM((anc * traits, 2 * mv), F32),
            pltpu.VMEM((2 * anc, 2 * mv), F32),
            part, part, part, part, part, part, part,
            pltpu.VMEM((2 * anc, mv), F32),
            pltpu.VMEM((2 * anc, mv), F32),
            pltpu.VMEM((anc * traits + anc, mv), F32),
            pltpu.VMEM((anc * traits + anc, mv), F32),
            dma, flags, dma, flags, dma, flags, dma, dma((chunks,)),
            dma, dma, dma, dma, dma((8,)),
        ],
        compiler_params=pltpu.CompilerParams(collective_id=0, has_side_effects=True, vmem_limit_bytes=LIMIT),
        name="em_step",
    )(genotypes, ancestry_counts.T, residuals.T, freqs)
    q_t, g_t, p_new, p_grad, z_flat = store(*results)
    return (q_t.T, g_t.T, p_new, p_grad, z_flat.reshape(anc, traits, mv))


def solution(mesh):
    in_specs = (
        P(("grp", "smp"), "var"),
        P(("grp", "smp"), None),
        P(("grp", "smp"), None),
        P("grp", "var"),
    )
    out_specs = (
        P(("grp", "smp", "var"), None),
        P(("grp", "smp", "var"), None),
        P("grp", "var"),
        P("grp", "var"),
        P("grp", None, "var"),
    )
    return jax.shard_map(shards, mesh=mesh, in_specs=in_specs, out_specs=out_specs, check_vma=False)
```

```python
import functools
import math

import jax
import jax.numpy as jnp
from jax import lax
from jax.experimental import pallas as pl
from jax.experimental.pallas import tpu as pltpu
from jax.sharding import PartitionSpec as P

MESH = pl.DeviceIdType.MESH
F32 = jnp.float32
BF16 = jnp.bfloat16
LIMIT = 67043328 - 491520
MOST = 5
NEAR_LAG = 3
OWN = 3
OTHER = 5
LAG = 3


def normalize(fractions, gradient, second):
    weighted = fractions * (gradient + second[:, None])
    return weighted / jnp.sum(weighted, axis=1, keepdims=True)


def update_freqs(freqs, excess_sum, second_sum, sample_count):
    allele_sum = excess_sum + second_sum
    freq_next = freqs * allele_sum / (freqs * allele_sum + (1.0 - freqs) * second_sum)
    freq_gradient = excess_sum * freqs.shape[0] / math.sqrt(sample_count)
    return (freq_next, freq_gradient)


def shards_plain(genotypes, ancestry_counts, residuals, freqs):
    highest = lax.Precision.HIGHEST
    var_count = lax.axis_size("var")
    sample_rows = genotypes.shape[0]
    sample_count = sample_rows * lax.axis_size("smp")
    variant_count = genotypes.shape[1] * var_count
    anc_count = freqs.shape[0]
    trait_count = residuals.shape[1]
    counts = ancestry_counts.astype(jnp.float32)
    fractions = counts / jnp.sum(counts, axis=1, keepdims=True)
    dosage = genotypes.astype(jnp.float32)
    recon_rows = jnp.dot(fractions, freqs, precision=highest)
    ratio_a = dosage / recon_rows
    ratio_b = (2.0 - dosage) / (1.0 - recon_rows)
    excess = ratio_a - ratio_b
    gradient_part = jnp.dot(excess, freqs.T, precision=highest)
    second_part = jnp.sum(ratio_b, axis=1)
    excess_part = jnp.dot(fractions.T, excess, precision=highest)
    return_part = jnp.dot(fractions.T, ratio_b, precision=highest)
    share_rows = sample_rows // var_count
    first_row = lax.axis_index("var") * share_rows
    excess_sum, second_sum = lax.psum((excess_part, return_part), "smp")
    freq_next, freq_gradient = update_freqs(freqs, excess_sum, second_sum, sample_count)
    gradient_all, second_all = lax.psum((gradient_part, second_part), "var")
    fraction_next = normalize(fractions, gradient_all, second_all)
    own_next = lax.dynamic_slice_in_dim(fraction_next, first_row, share_rows, 0)
    own_gradient = lax.dynamic_slice_in_dim(gradient_all, first_row, share_rows, 0)
    scaled_gradient = own_gradient / math.sqrt(variant_count)
    ratio_next = dosage / jnp.dot(fraction_next, freqs, precision=highest)
    residual = residuals.astype(jnp.float32) / 1000.0
    trait_rows = (fraction_next[:, :, None] * residual[:, None, :]).reshape(
        sample_rows, anc_count * trait_count
    )
    score_part = jnp.dot(trait_rows.T, ratio_next, precision=highest)
    info_part = jnp.dot(
        (fraction_next * fraction_next).T, ratio_next * ratio_next, precision=highest
    )
    score_sum, info_sum = lax.psum((score_part, info_part), "smp")
    score_tiles = score_sum.reshape(anc_count, trait_count, genotypes.shape[1])
    z_score = score_tiles / jnp.sqrt(info_sum + 1e-06)[:, None, :]
    return (own_next, scaled_gradient, freq_next, freq_gradient, z_score)


def split(x):
    high = x.astype(BF16)
    return high, (x - high.astype(F32)).astype(BF16)


def dot(a, b):
    return jnp.dot(a, b, preferred_element_type=F32)


def dot_lanes(a, b):
    return lax.dot_general(a, b, (((1,), (1,)), ((), ())), preferred_element_type=F32)


def kernel(
    dims,
    geno_in, counts_in, resid_in, freqs_in,
    q_out, g_out, p_out, pg_out, z_out,
    geno, counts, resid, freqs, fstack, qf, gf, fcol, frow, ebuf, tbuf,
    acc_ex, acc_sc, acc_in,
    xs, xr, zs, er, mr, go, gp, fs, fr, ss, sr,
    xs_s, xs_r, z_s, z_r, m_s, m_r, xa_s, xa_r, f_s, f_r, s_s, s_r, in_s,
):
    chunks, width, half, own_per, per, variant_count, sample_count, share, var_n = dims
    sub = width // 128
    anc = freqs.shape[0]
    traits = resid.shape[0]
    mv = freqs.shape[1]
    me = lax.axis_index("var")
    core = lax.axis_index("smp")
    x = lax.rem(me, 2)
    z = me // 2
    zn = z + 1 - 2 * lax.rem(z, 2)
    middle = jnp.logical_or(z == 1, z == 2)
    end = jnp.logical_or(z == 0, z == 3)
    partner = {"var": z * 2 + (1 - x)}
    twin = {"smp": 1 - core}
    beside = {"var": zn * 2 + x}
    across = {"var": lax.rem(7 - z, 4) * 2 + x}

    def load(src, dst, which, base=None, size=None):
        if base is not None:
            src, dst = src.at[pl.ds(base, size), :], dst.at[pl.ds(base, size), :]
        return pltpu.make_async_copy(src, dst, in_s.at[which])

    def load_lanes(src, dst, which, base, size):
        return pltpu.make_async_copy(
            src.at[:, pl.ds(base, size)], dst.at[:, pl.ds(base, size)], in_s.at[which]
        )

    far_half = pl.multiple_of((1 - x) * half, 128)
    near_half = pl.multiple_of(x * half, 128)
    freqs_load = load(freqs_in, freqs, 0)
    first_loads = (
        load_lanes(counts_in, counts, 1, far_half, width),
        load(geno_in, geno, 2, far_half, width),
    )
    later_loads = ()
    if chunks > 1:
        far_next = pl.multiple_of(far_half + width, 128)
        later_loads = (
            load_lanes(counts_in, counts, 3, far_next, half - width),
            load(geno_in, geno, 4, far_next, half - width),
        )
    near_loads = (
        load_lanes(counts_in, counts, 5, near_half, half),
        load(geno_in, geno, 6, near_half, half),
    )
    resid_load = load(resid_in, resid, 7)
    for item in (freqs_load,) + first_loads + later_loads + near_loads + (resid_load,):
        item.start()

    barrier = pltpu.get_barrier_semaphore()
    for peer in (partner, twin, beside):
        pl.semaphore_signal(barrier, inc=1, device_id=peer, device_id_type=MESH)

    @pl.when(middle)
    def _():
        pl.semaphore_signal(barrier, inc=1, device_id=across, device_id_type=MESH)

    acc_ex[...] = jnp.zeros_like(acc_ex)
    acc_sc[...] = jnp.zeros_like(acc_sc)
    acc_in[...] = jnp.zeros_like(acc_in)
    freqs_load.wait()
    p = freqs[...]
    p_hi, p_lo = split(p)
    stack = jnp.concatenate([p_hi.astype(F32), p_lo.astype(F32)] * 2, axis=0)
    fcol[...] = stack.T.astype(BF16)
    fstack[...] = stack.astype(BF16)
    frow[0:anc, 0:mv] = p_hi
    frow[0:anc, mv:] = p_hi
    frow[anc:, 0:mv] = p_lo
    frow[anc:, mv:] = p_lo

    def lanes(which, c):
        return pl.multiple_of(which * half + c * width, 128)

    def first_pass(off):
        d = geno[pl.ds(off, width), :].astype(F32).T
        c = counts[:, pl.ds(off, width)].astype(F32)
        total = jnp.sum(c, axis=0, keepdims=True)
        cb = c.astype(BF16)
        none = jnp.zeros_like(cb)
        u = dot(fcol[...], jnp.concatenate([cb, cb, none, none], axis=0))
        w = total - u
        inverse = 1.0 / (u * w)
        b = (2.0 - d) * u * inverse
        e = d * w * inverse - b
        e_hi, e_lo = split(e)
        b_hi, b_lo = split(b)
        ebuf[0:mv, :] = e_hi
        ebuf[mv : 2 * mv, :] = e_lo
        ebuf[2 * mv : 3 * mv, :] = b_hi
        ebuf[3 * mv :, :] = b_lo
        g = dot(frow[...], ebuf[0 : 2 * mv, :])
        acc_ex[...] += dot_lanes(ebuf[...], jnp.concatenate([cb] * (128 // anc), axis=0))
        return (g[0:anc, :] + g[anc:, :]) * total

    def second_pass(off, g):
        width = g.shape[1]
        c = counts[:, pl.ds(off, width)].astype(F32)
        f = c / jnp.sum(c, axis=0, keepdims=True)
        second = 2.0 * variant_count - jnp.sum(f * g, axis=0, keepdims=True)
        weighted = f * (g + second)
        q = weighted / jnp.sum(weighted, axis=0, keepdims=True)
        qf[:, pl.ds(off, width)] = q
        gf[:, pl.ds(off, width)] = g * (1.0 / math.sqrt(variant_count))
        q_hi, q_lo = split(q)
        recon = lax.dot_general(
            jnp.concatenate([q_hi, q_hi, q_lo, q_lo], axis=0),
            fstack[...],
            (((0,), (0,)), ((), ())),
            preferred_element_type=F32,
        )
        r = geno[pl.ds(off, width), :].astype(F32) / recon
        r_hi, r_lo = split(r)
        s_hi, s_lo = split(r * r)
        t = resid[:, pl.ds(off, width)].astype(F32)
        r_cat = jnp.concatenate([r_hi, r_lo], axis=1)
        r_cat = jnp.concatenate([r_cat, r_cat], axis=0)
        step = anc // 2
        for m in range(2):
            for k in range(step * m, step * (m + 1)):
                t_hi, t_lo = split(q[k : k + 1, :] * t)
                tbuf[traits * k : traits * (k + 1), 0:width] = t_hi
                tbuf[traits * k : traits * (k + 1), width : 2 * width] = t_lo
            at = slice(traits * step * m, traits * step * (m + 1))
            o = dot(tbuf[at, 0 : 2 * width], r_cat)
            acc_sc[at, :] += o[:, 0:mv] + o[:, mv:]
        y_hi, y_lo = split(q * q)
        none = jnp.zeros_like(y_hi)
        acc_in[...] += dot(
            jnp.concatenate([y_hi, y_lo], axis=0), jnp.concatenate([s_hi, s_lo], axis=1)
        )

    def copy(src, dst, send, recv, peer):
        return pltpu.make_async_remote_copy(
            src_ref=src, dst_ref=dst, send_sem=send, recv_sem=recv, device_id=peer, device_id_type=MESH
        )

    def x_reduce(t):
        return copy(xs.at[t], xr.at[t], xs_s, xs_r.at[t], partner)

    def inward(t):
        return copy(zs.at[t], er.at[t], z_s, z_r.at[t], beside)

    def exchange(t):
        return copy(zs.at[t], mr.at[t], m_s, m_r.at[t], across)

    def outward(t):
        return copy(go.at[t], go.at[t], z_s, z_r.at[t], beside)

    def x_gather(t):
        return copy(go.at[t], gp.at[t], xa_s, xa_r.at[t // per], partner)

    def x_gathered(c):
        at = pl.ds(c * per, per)
        return copy(go.at[at], gp.at[at], xa_s, xa_r.at[c], partner)

    def put(ref, c, g):
        for j in range(sub):
            ref[c * sub + j] = g[:, 128 * j : 128 * (j + 1)]

    def take(ref, at, count):
        return jnp.concatenate([ref[at + j] for j in range(count)], axis=1)

    for item in first_loads:
        item.wait()
    put(xs, 0, first_pass(lanes(1 - x, 0)))

    @pl.when(middle)
    def _():
        pl.semaphore_wait(barrier, 4)

    @pl.when(end)
    def _():
        pl.semaphore_wait(barrier, 3)

    for j in range(sub):
        x_reduce(j).start()
    for item in later_loads:
        item.wait()

    def step_far(c, carry):
        put(xs, c, first_pass(lanes(1 - x, c)))
        for j in range(sub):
            x_reduce(c * sub + j).start()
        return carry

    lax.fori_loop(1, chunks, step_far, 0)
    for item in near_loads:
        item.wait()

    def add_inward(t):
        inward(t).wait_recv()
        zs[t] = zs[t] + er[t]
        exchange(t).start()

    def add_exchange(c, j):
        t = c * sub + j
        exchange(t).wait_recv()
        go[t] = zs[t] + mr[t]
        outward(t).start()
        x_gather(t).start()

    def step_near(c, carry):
        put(zs, c, first_pass(lanes(x, c)))
        for j in range(sub):
            t = c * sub + j
            x_reduce(t).wait_recv()
            zs[t] = zs[t] + xr[t]

            @pl.when(end)
            def _(t=t):
                inward(t).start()

            @pl.when(jnp.logical_and(middle, c >= NEAR_LAG))
            def _(t=t):
                add_inward(t - NEAR_LAG * sub)

        return carry

    lax.fori_loop(0, chunks, step_near, 0)

    ex = acc_ex[0:mv, :] + acc_ex[mv : 2 * mv, :]
    re = acc_ex[2 * mv : 3 * mv, :] + acc_ex[3 * mv :, :]
    fs[0:anc, :] = ex.T[0:anc, :]
    fs[anc:, :] = re.T[0:anc, :]
    freq_copy = copy(fs, fr, f_s, f_r, twin)
    freq_copy.start()

    @pl.when(middle)
    def _():
        def step_inward(t, carry):
            add_inward(t)
            return carry

        def step_exchange(c, carry):
            for j in range(sub):
                t = c * sub + j

                @pl.when(c + LAG < chunks)
                def _(t=t):
                    add_inward(t + LAG * sub)

                add_exchange(c, j)
            return carry

        lax.fori_loop(max(0, chunks - NEAR_LAG) * sub, min(LAG, chunks) * sub, step_inward, 0)
        lax.fori_loop(0, chunks, step_exchange, 0)

    resid_load.wait()

    def step_own(c, carry):
        for j in range(own_per):
            t = c * own_per + j

            @pl.when(end)
            def _(t=t):
                outward(t).wait_recv()
                x_gather(t).start()

        second_pass(pl.multiple_of(x * half + c * own_per * 128, 128), take(go, c * own_per, own_per))
        return carry

    lax.fori_loop(0, chunks * sub // own_per, step_own, 0)

    def step_other(c, carry):
        x_gathered(c).wait_recv()
        second_pass(pl.multiple_of((1 - x) * half + c * per * 128, 128), take(gp, c * per, per))
        return carry

    lax.fori_loop(0, chunks * sub // per, step_other, 0)

    tiles = anc * traits
    ss[0:tiles, :] = acc_sc[...]
    info = acc_in[0:anc, :] + acc_in[anc:, :]
    ss[tiles:, :] = info[:, 0:mv] + info[:, mv:]
    score_copy = copy(ss, sr, s_s, s_r, twin)
    score_copy.start()

    freq_copy.wait_recv()
    sums = fs[...] + fr[...]
    excess_sum = sums[0:anc, :]
    second_sum = sums[anc:, :]
    freq_next, freq_gradient = update_freqs(freqs[...], excess_sum, second_sum, sample_count)
    p_out[...] = freq_next
    pg_out[...] = freq_gradient

    for v in range(var_n):

        @pl.when(me == v)
        def _():
            q_out[...] = qf[:, share * v : share * (v + 1)]
            g_out[...] = gf[:, share * v : share * (v + 1)]

    copy(xs, xr, xs_s, xs_r.at[0], partner).wait_send()
    copy(go, gp, xa_s, xa_r.at[0], partner).wait_send()
    copy(zs, er, z_s, z_r.at[0], beside).wait_send()

    @pl.when(middle)
    def _():
        copy(zs, mr, m_s, m_r.at[0], across).wait_send()

    freq_copy.wait_send()
    score_copy.wait_recv()
    info_sum = ss[tiles:, :] + sr[tiles:, :]
    scale = 0.001 / jnp.sqrt(info_sum + 1e-06)
    for k in range(anc):
        at = slice(traits * k, traits * (k + 1))
        z_out[at, :] = (ss[at, :] + sr[at, :]) * scale[k : k + 1, :]
    score_copy.wait_send()


def store_kernel(*refs):
    count = len(refs) // 2
    sems = refs[-1]
    copies = [pltpu.make_async_copy(refs[i], refs[count + i], sems.at[i]) for i in range(count)]
    for item in copies:
        item.start()
    for item in copies:
        item.wait()


def store(*arrays):
    return pl.pallas_call(
        store_kernel,
        out_shape=tuple(jax.ShapeDtypeStruct(a.shape, a.dtype) for a in arrays),
        in_specs=[pl.BlockSpec(memory_space=pltpu.VMEM)] * len(arrays),
        out_specs=(pl.BlockSpec(memory_space=pl.ANY),) * len(arrays),
        scratch_shapes=[pltpu.SemaphoreType.DMA((len(arrays),))],
        compiler_params=pltpu.CompilerParams(vmem_limit_bytes=1024 * 1024),
        name="store",
    )(*arrays)


def fits(genotypes, residuals, freqs, var_n):
    samples, mv = genotypes.shape
    anc = freqs.shape[0]
    return (
        var_n == 8
        and lax.axis_size("smp") == 2
        and anc == 32
        and mv == 128
        and residuals.shape[1] % 16 == 0
        and samples % (2 * 128) == 0
        and samples % var_n == 0
    )


def shards(genotypes, ancestry_counts, residuals, freqs):
    var_n = lax.axis_size("var")
    if not fits(genotypes, residuals, freqs, var_n):
        return shards_plain(genotypes, ancestry_counts, residuals, freqs)
    samples, mv = genotypes.shape
    anc = freqs.shape[0]
    traits = residuals.shape[1]
    half = samples // 2
    tiles = half // 128
    chunks = max(n for n in range(1, MOST + 1) if tiles % n == 0)
    width = half // chunks
    own_per = max(n for n in range(1, OWN + 1) if tiles % n == 0)
    per = max(n for n in range(1, OTHER + 1) if tiles % n == 0)
    share = samples // var_n
    dims = (chunks, width, half, own_per, per, mv * var_n, samples * lax.axis_size("smp"), share, var_n)
    vmem = pl.BlockSpec(memory_space=pltpu.VMEM)
    dma = pltpu.SemaphoreType.DMA
    part = pltpu.VMEM((half // 128, anc, 128), F32)
    flags = dma((half // 128,))
    results = pl.pallas_call(
        functools.partial(kernel, dims),
        out_shape=(
            pltpu.VMEM((anc, share), F32),
            pltpu.VMEM((anc, share), F32),
            pltpu.VMEM((anc, mv), F32),
            pltpu.VMEM((anc, mv), F32),
            pltpu.VMEM((anc * traits, mv), F32),
        ),
        in_specs=[pl.BlockSpec(memory_space=pltpu.HBM)] * 4,
        out_specs=(vmem,) * 5,
        scratch_shapes=[
            pltpu.VMEM((samples, mv), BF16),
            pltpu.VMEM((anc, samples), jnp.int32),
            pltpu.VMEM((traits, samples), jnp.int32),
            pltpu.VMEM((anc, mv), F32),
            pltpu.VMEM((4 * anc, mv), BF16),
            pltpu.VMEM((anc, samples), F32),
            pltpu.VMEM((anc, samples), F32),
            pltpu.VMEM((mv, 4 * anc), BF16),
            pltpu.VMEM((2 * anc, 2 * mv), BF16),
            pltpu.VMEM((4 * mv, width), BF16),
            pltpu.VMEM((anc * traits, 256 * max(own_per, per)), BF16),
            pltpu.VMEM((4 * mv, 128), F32),
            pltpu.VMEM((anc * traits, mv), F32),
            pltpu.VMEM((2 * anc, 2 * mv), F32),
            part, part, part, part, part, part, part,
            pltpu.VMEM((2 * anc, mv), F32),
            pltpu.VMEM((2 * anc, mv), F32),
            pltpu.VMEM((anc * traits + anc, mv), F32),
            pltpu.VMEM((anc * traits + anc, mv), F32),
            dma, flags, dma, flags, dma, flags, dma, dma((tiles // per,)),
            dma, dma, dma, dma, dma((8,)),
        ],
        compiler_params=pltpu.CompilerParams(collective_id=0, has_side_effects=True, vmem_limit_bytes=LIMIT),
        name="em_step",
    )(genotypes, ancestry_counts.T, residuals.T, freqs)
    q_t, g_t, p_new, p_grad, z_flat = store(*results)
    return (q_t.T, g_t.T, p_new, p_grad, z_flat.reshape(anc, traits, mv))


def solution(mesh):
    in_specs = (
        P(("grp", "smp"), "var"),
        P(("grp", "smp"), None),
        P(("grp", "smp"), None),
        P("grp", "var"),
    )
    out_specs = (
        P(("grp", "smp", "var"), None),
        P(("grp", "smp", "var"), None),
        P("grp", "var"),
        P("grp", "var"),
        P("grp", None, "var"),
    )
    return jax.shard_map(shards, mesh=mesh, in_specs=in_specs, out_specs=out_specs, check_vma=False)
```

```python
import functools
import math

import jax
import jax.numpy as jnp
from jax import lax
from jax.experimental import pallas as pl
from jax.experimental.pallas import tpu as pltpu
from jax.sharding import PartitionSpec as P

MESH = pl.DeviceIdType.MESH
F32 = jnp.float32
BF16 = jnp.bfloat16
LIMIT = 67043328 - 491520
MOST = 5
NEAR_LAG = 3
OWN = 3
OTHER = 5
LAG = 3


def normalize(fractions, gradient, second):
    weighted = fractions * (gradient + second[:, None])
    return weighted / jnp.sum(weighted, axis=1, keepdims=True)


def update_freqs(freqs, excess_sum, second_sum, sample_count):
    allele_sum = excess_sum + second_sum
    freq_next = freqs * allele_sum / (freqs * allele_sum + (1.0 - freqs) * second_sum)
    freq_gradient = excess_sum * freqs.shape[0] / math.sqrt(sample_count)
    return (freq_next, freq_gradient)


def shards_plain(genotypes, ancestry_counts, residuals, freqs):
    highest = lax.Precision.HIGHEST
    var_count = lax.axis_size("var")
    sample_rows = genotypes.shape[0]
    sample_count = sample_rows * lax.axis_size("smp")
    variant_count = genotypes.shape[1] * var_count
    anc_count = freqs.shape[0]
    trait_count = residuals.shape[1]
    counts = ancestry_counts.astype(jnp.float32)
    fractions = counts / jnp.sum(counts, axis=1, keepdims=True)
    dosage = genotypes.astype(jnp.float32)
    recon_rows = jnp.dot(fractions, freqs, precision=highest)
    ratio_a = dosage / recon_rows
    ratio_b = (2.0 - dosage) / (1.0 - recon_rows)
    excess = ratio_a - ratio_b
    gradient_part = jnp.dot(excess, freqs.T, precision=highest)
    second_part = jnp.sum(ratio_b, axis=1)
    excess_part = jnp.dot(fractions.T, excess, precision=highest)
    return_part = jnp.dot(fractions.T, ratio_b, precision=highest)
    share_rows = sample_rows // var_count
    first_row = lax.axis_index("var") * share_rows
    excess_sum, second_sum = lax.psum((excess_part, return_part), "smp")
    freq_next, freq_gradient = update_freqs(freqs, excess_sum, second_sum, sample_count)
    gradient_all, second_all = lax.psum((gradient_part, second_part), "var")
    fraction_next = normalize(fractions, gradient_all, second_all)
    own_next = lax.dynamic_slice_in_dim(fraction_next, first_row, share_rows, 0)
    own_gradient = lax.dynamic_slice_in_dim(gradient_all, first_row, share_rows, 0)
    scaled_gradient = own_gradient / math.sqrt(variant_count)
    ratio_next = dosage / jnp.dot(fraction_next, freqs, precision=highest)
    residual = residuals.astype(jnp.float32) / 1000.0
    trait_rows = (fraction_next[:, :, None] * residual[:, None, :]).reshape(
        sample_rows, anc_count * trait_count
    )
    score_part = jnp.dot(trait_rows.T, ratio_next, precision=highest)
    info_part = jnp.dot(
        (fraction_next * fraction_next).T, ratio_next * ratio_next, precision=highest
    )
    score_sum, info_sum = lax.psum((score_part, info_part), "smp")
    score_tiles = score_sum.reshape(anc_count, trait_count, genotypes.shape[1])
    z_score = score_tiles / jnp.sqrt(info_sum + 1e-06)[:, None, :]
    return (own_next, scaled_gradient, freq_next, freq_gradient, z_score)


def split(x):
    high = x.astype(BF16)
    return high, (x - high.astype(F32)).astype(BF16)


def dot(a, b):
    return jnp.dot(a, b, preferred_element_type=F32)


def dot_lanes(a, b):
    return lax.dot_general(a, b, (((1,), (1,)), ((), ())), preferred_element_type=F32)


def kernel(
    dims,
    geno_in, counts_in, resid_in, freqs_in,
    q_out, g_out, p_out, pg_out, z_out,
    geno, counts, resid, freqs, fstack, qf, gf, fcol, frow, ebuf, tbuf,
    acc_ex, acc_sc, acc_in,
    xs, xr, zs, er, mr, go, gp, fs, fr, ss, sr,
    xs_s, xs_r, z_s, z_r, m_s, m_r, xa_s, xa_r, f_s, f_r, s_s, s_r, in_s,
):
    chunks, width, half, own_per, per, variant_count, sample_count, share, var_n = dims
    sub = width // 128
    anc = freqs.shape[0]
    traits = resid.shape[0]
    mv = freqs.shape[1]
    me = lax.axis_index("var")
    core = lax.axis_index("smp")
    x = lax.rem(me, 2)
    z = me // 2
    zn = z + 1 - 2 * lax.rem(z, 2)
    middle = jnp.logical_or(z == 1, z == 2)
    end = jnp.logical_or(z == 0, z == 3)
    partner = {"var": z * 2 + (1 - x)}
    twin = {"smp": 1 - core}
    beside = {"var": zn * 2 + x}
    across = {"var": lax.rem(7 - z, 4) * 2 + x}

    def load(src, dst, which, base=None, size=None):
        if base is not None:
            src, dst = src.at[pl.ds(base, size), :], dst.at[pl.ds(base, size), :]
        return pltpu.make_async_copy(src, dst, in_s.at[which])

    def load_lanes(src, dst, which, base, size):
        return pltpu.make_async_copy(
            src.at[:, pl.ds(base, size)], dst.at[:, pl.ds(base, size)], in_s.at[which]
        )

    far_half = pl.multiple_of((1 - x) * half, 128)
    near_half = pl.multiple_of(x * half, 128)
    freqs_load = load(freqs_in, freqs, 0)
    first_loads = (
        load_lanes(counts_in, counts, 1, far_half, width),
        load(geno_in, geno, 2, far_half, width),
    )
    later_loads = ()
    if chunks > 1:
        far_next = pl.multiple_of(far_half + width, 128)
        later_loads = (
            load_lanes(counts_in, counts, 3, far_next, half - width),
            load(geno_in, geno, 4, far_next, half - width),
        )
    near_loads = (
        load_lanes(counts_in, counts, 5, near_half, half),
        load(geno_in, geno, 6, near_half, half),
    )
    resid_load = load(resid_in, resid, 7)
    for item in (freqs_load,) + first_loads + later_loads + near_loads + (resid_load,):
        item.start()

    barrier = pltpu.get_barrier_semaphore()
    for peer in (partner, twin, beside):
        pl.semaphore_signal(barrier, inc=1, device_id=peer, device_id_type=MESH)

    @pl.when(middle)
    def _():
        pl.semaphore_signal(barrier, inc=1, device_id=across, device_id_type=MESH)

    acc_ex[...] = jnp.zeros_like(acc_ex)
    acc_sc[...] = jnp.zeros_like(acc_sc)
    acc_in[...] = jnp.zeros_like(acc_in)
    freqs_load.wait()
    p = freqs[...]
    p_hi, p_lo = split(p)
    stack = jnp.concatenate([p_hi.astype(F32), p_lo.astype(F32)] * 2, axis=0)
    fcol[...] = stack.T.astype(BF16)
    fstack[...] = stack.astype(BF16)
    frow[0:anc, 0:mv] = p_hi
    frow[0:anc, mv:] = p_hi
    frow[anc:, 0:mv] = p_lo
    frow[anc:, mv:] = p_lo

    def lanes(which, c):
        return pl.multiple_of(which * half + c * width, 128)

    def first_pass(off):
        d = geno[pl.ds(off, width), :].astype(F32).T
        c = counts[:, pl.ds(off, width)].astype(F32)
        total = jnp.sum(c, axis=0, keepdims=True)
        cb = c.astype(BF16)
        none = jnp.zeros_like(cb)
        u = dot(fcol[...], jnp.concatenate([cb, cb, none, none], axis=0))
        w = total - u
        inverse = 1.0 / (u * w)
        b = (2.0 - d) * u * inverse
        e = d * w * inverse - b
        e_hi, e_lo = split(e)
        b_hi, b_lo = split(b)
        ebuf[0:mv, :] = e_hi
        ebuf[mv : 2 * mv, :] = e_lo
        ebuf[2 * mv : 3 * mv, :] = b_hi
        ebuf[3 * mv :, :] = b_lo
        g = dot(frow[...], ebuf[0 : 2 * mv, :])
        acc_ex[...] += dot_lanes(ebuf[...], jnp.concatenate([cb] * (128 // anc), axis=0))
        return (g[0:anc, :] + g[anc:, :]) * total

    def second_pass(off, g):
        width = g.shape[1]
        c = counts[:, pl.ds(off, width)].astype(F32)
        f = c / jnp.sum(c, axis=0, keepdims=True)
        second = 2.0 * variant_count - jnp.sum(f * g, axis=0, keepdims=True)
        weighted = f * (g + second)
        q = weighted / jnp.sum(weighted, axis=0, keepdims=True)
        qf[:, pl.ds(off, width)] = q
        gf[:, pl.ds(off, width)] = g * (1.0 / math.sqrt(variant_count))
        q_hi, q_lo = split(q)
        recon = lax.dot_general(
            jnp.concatenate([q_hi, q_hi, q_lo, q_lo], axis=0),
            fstack[...],
            (((0,), (0,)), ((), ())),
            preferred_element_type=F32,
        )
        r = geno[pl.ds(off, width), :].astype(F32) / recon
        r_hi, r_lo = split(r)
        s_hi, s_lo = split(r * r)
        t = resid[:, pl.ds(off, width)].astype(F32)
        r_cat = jnp.concatenate([r_hi, r_lo], axis=1)
        r_cat = jnp.concatenate([r_cat, r_cat], axis=0)
        step = anc // 2
        for m in range(2):
            for k in range(step * m, step * (m + 1)):
                t_hi, t_lo = split(q[k : k + 1, :] * t)
                tbuf[traits * k : traits * (k + 1), 0:width] = t_hi
                tbuf[traits * k : traits * (k + 1), width : 2 * width] = t_lo
            at = slice(traits * step * m, traits * step * (m + 1))
            o = dot(tbuf[at, 0 : 2 * width], r_cat)
            acc_sc[at, :] += o[:, 0:mv] + o[:, mv:]
        y_hi, y_lo = split(q * q)
        none = jnp.zeros_like(y_hi)
        acc_in[...] += dot(
            jnp.concatenate([y_hi, y_lo], axis=0), jnp.concatenate([s_hi, s_lo], axis=1)
        )

    def copy(src, dst, send, recv, peer):
        return pltpu.make_async_remote_copy(
            src_ref=src, dst_ref=dst, send_sem=send, recv_sem=recv, device_id=peer, device_id_type=MESH
        )

    def x_reduce(t):
        return copy(xs.at[t], xr.at[t], xs_s, xs_r.at[t], partner)

    def inward(t):
        return copy(zs.at[t], er.at[t], z_s, z_r.at[t], beside)

    def exchange(t):
        return copy(zs.at[t], mr.at[t], m_s, m_r.at[t], across)

    def outward(t):
        return copy(go.at[t], go.at[t], z_s, z_r.at[t], beside)

    def x_gather(t):
        return copy(go.at[t], gp.at[t], xa_s, xa_r.at[t // per], partner)

    def x_gathered(c):
        at = pl.ds(c * per, per)
        return copy(go.at[at], gp.at[at], xa_s, xa_r.at[c], partner)

    def put(ref, c, g):
        for j in range(sub):
            ref[c * sub + j] = g[:, 128 * j : 128 * (j + 1)]

    def take(ref, at, count):
        return jnp.concatenate([ref[at + j] for j in range(count)], axis=1)

    for item in first_loads:
        item.wait()
    put(xs, 0, first_pass(lanes(1 - x, 0)))

    @pl.when(middle)
    def _():
        pl.semaphore_wait(barrier, 4)

    @pl.when(end)
    def _():
        pl.semaphore_wait(barrier, 3)

    for j in range(sub):
        x_reduce(j).start()
    for item in later_loads:
        item.wait()

    def step_far(c, carry):
        put(xs, c, first_pass(lanes(1 - x, c)))
        for j in range(sub):
            x_reduce(c * sub + j).start()
        return carry

    lax.fori_loop(1, chunks, step_far, 0)
    for item in near_loads:
        item.wait()

    def add_inward(t):
        inward(t).wait_recv()
        zs[t] = zs[t] + er[t]
        exchange(t).start()

    def add_exchange(c, j):
        t = c * sub + j
        exchange(t).wait_recv()
        go[t] = zs[t] + mr[t]
        outward(t).start()
        x_gather(t).start()

    def step_near(c, carry):
        put(zs, c, first_pass(lanes(x, c)))
        for j in range(sub):
            t = c * sub + j
            x_reduce(t).wait_recv()
            zs[t] = zs[t] + xr[t]

            @pl.when(end)
            def _(t=t):
                inward(t).start()

            @pl.when(jnp.logical_and(middle, c >= NEAR_LAG))
            def _(t=t):
                add_inward(t - NEAR_LAG * sub)

        return carry

    lax.fori_loop(0, chunks, step_near, 0)

    ex = acc_ex[0:mv, :] + acc_ex[mv : 2 * mv, :]
    re = acc_ex[2 * mv : 3 * mv, :] + acc_ex[3 * mv :, :]
    fs[0:anc, :] = ex.T[0:anc, :]
    fs[anc:, :] = re.T[0:anc, :]
    freq_copy = copy(fs, fr, f_s, f_r, twin)
    freq_copy.start()

    @pl.when(middle)
    def _():
        def step_inward(t, carry):
            add_inward(t)
            return carry

        def step_exchange(c, carry):
            for j in range(sub):
                t = c * sub + j

                @pl.when(c + LAG < chunks)
                def _(t=t):
                    add_inward(t + LAG * sub)

                add_exchange(c, j)
            return carry

        for t in range(max(0, chunks - NEAR_LAG) * sub, min(LAG, chunks) * sub):
            step_inward(t, 0)
        for c in range(chunks):
            step_exchange(c, 0)

    resid_load.wait()

    def step_own(c, carry):
        for j in range(own_per):
            t = c * own_per + j

            @pl.when(end)
            def _(t=t):
                outward(t).wait_recv()
                x_gather(t).start()

        second_pass(pl.multiple_of(x * half + c * own_per * 128, 128), take(go, c * own_per, own_per))
        return carry

    lax.fori_loop(0, chunks * sub // own_per, step_own, 0)

    def step_other(c, carry):
        x_gathered(c).wait_recv()
        second_pass(pl.multiple_of((1 - x) * half + c * per * 128, 128), take(gp, c * per, per))
        return carry

    lax.fori_loop(0, chunks * sub // per, step_other, 0)

    tiles = anc * traits
    ss[0:tiles, :] = acc_sc[...]
    info = acc_in[0:anc, :] + acc_in[anc:, :]
    ss[tiles:, :] = info[:, 0:mv] + info[:, mv:]
    score_copy = copy(ss, sr, s_s, s_r, twin)
    score_copy.start()

    freq_copy.wait_recv()
    sums = fs[...] + fr[...]
    excess_sum = sums[0:anc, :]
    second_sum = sums[anc:, :]
    freq_next, freq_gradient = update_freqs(freqs[...], excess_sum, second_sum, sample_count)
    p_out[...] = freq_next
    pg_out[...] = freq_gradient

    for v in range(var_n):

        @pl.when(me == v)
        def _():
            q_out[...] = qf[:, share * v : share * (v + 1)]
            g_out[...] = gf[:, share * v : share * (v + 1)]

    copy(xs, xr, xs_s, xs_r.at[0], partner).wait_send()
    copy(go, gp, xa_s, xa_r.at[0], partner).wait_send()
    copy(zs, er, z_s, z_r.at[0], beside).wait_send()

    @pl.when(middle)
    def _():
        copy(zs, mr, m_s, m_r.at[0], across).wait_send()

    freq_copy.wait_send()
    score_copy.wait_recv()
    info_sum = ss[tiles:, :] + sr[tiles:, :]
    scale = 0.001 / jnp.sqrt(info_sum + 1e-06)
    for k in range(anc):
        at = slice(traits * k, traits * (k + 1))
        z_out[at, :] = (ss[at, :] + sr[at, :]) * scale[k : k + 1, :]
    score_copy.wait_send()


def store_kernel(*refs):
    count = len(refs) // 2
    sems = refs[-1]
    copies = [pltpu.make_async_copy(refs[i], refs[count + i], sems.at[i]) for i in range(count)]
    for item in copies:
        item.start()
    for item in copies:
        item.wait()


def store(*arrays):
    return pl.pallas_call(
        store_kernel,
        out_shape=tuple(jax.ShapeDtypeStruct(a.shape, a.dtype) for a in arrays),
        in_specs=[pl.BlockSpec(memory_space=pltpu.VMEM)] * len(arrays),
        out_specs=(pl.BlockSpec(memory_space=pl.ANY),) * len(arrays),
        scratch_shapes=[pltpu.SemaphoreType.DMA((len(arrays),))],
        compiler_params=pltpu.CompilerParams(vmem_limit_bytes=1024 * 1024),
        name="store",
    )(*arrays)


def fits(genotypes, residuals, freqs, var_n):
    samples, mv = genotypes.shape
    anc = freqs.shape[0]
    return (
        var_n == 8
        and lax.axis_size("smp") == 2
        and anc == 32
        and mv == 128
        and residuals.shape[1] % 16 == 0
        and samples % (2 * 128) == 0
        and samples % var_n == 0
    )


def shards(genotypes, ancestry_counts, residuals, freqs):
    var_n = lax.axis_size("var")
    if not fits(genotypes, residuals, freqs, var_n):
        return shards_plain(genotypes, ancestry_counts, residuals, freqs)
    samples, mv = genotypes.shape
    anc = freqs.shape[0]
    traits = residuals.shape[1]
    half = samples // 2
    tiles = half // 128
    chunks = max(n for n in range(1, MOST + 1) if tiles % n == 0)
    width = half // chunks
    own_per = max(n for n in range(1, OWN + 1) if tiles % n == 0)
    per = max(n for n in range(1, OTHER + 1) if tiles % n == 0)
    share = samples // var_n
    dims = (chunks, width, half, own_per, per, mv * var_n, samples * lax.axis_size("smp"), share, var_n)
    vmem = pl.BlockSpec(memory_space=pltpu.VMEM)
    dma = pltpu.SemaphoreType.DMA
    part = pltpu.VMEM((half // 128, anc, 128), F32)
    flags = dma((half // 128,))
    results = pl.pallas_call(
        functools.partial(kernel, dims),
        out_shape=(
            pltpu.VMEM((anc, share), F32),
            pltpu.VMEM((anc, share), F32),
            pltpu.VMEM((anc, mv), F32),
            pltpu.VMEM((anc, mv), F32),
            pltpu.VMEM((anc * traits, mv), F32),
        ),
        in_specs=[pl.BlockSpec(memory_space=pltpu.HBM)] * 4,
        out_specs=(vmem,) * 5,
        scratch_shapes=[
            pltpu.VMEM((samples, mv), BF16),
            pltpu.VMEM((anc, samples), jnp.int32),
            pltpu.VMEM((traits, samples), jnp.int32),
            pltpu.VMEM((anc, mv), F32),
            pltpu.VMEM((4 * anc, mv), BF16),
            pltpu.VMEM((anc, samples), F32),
            pltpu.VMEM((anc, samples), F32),
            pltpu.VMEM((mv, 4 * anc), BF16),
            pltpu.VMEM((2 * anc, 2 * mv), BF16),
            pltpu.VMEM((4 * mv, width), BF16),
            pltpu.VMEM((anc * traits, 256 * max(own_per, per)), BF16),
            pltpu.VMEM((4 * mv, 128), F32),
            pltpu.VMEM((anc * traits, mv), F32),
            pltpu.VMEM((2 * anc, 2 * mv), F32),
            part, part, part, part, part, part, part,
            pltpu.VMEM((2 * anc, mv), F32),
            pltpu.VMEM((2 * anc, mv), F32),
            pltpu.VMEM((anc * traits + anc, mv), F32),
            pltpu.VMEM((anc * traits + anc, mv), F32),
            dma, flags, dma, flags, dma, flags, dma, dma((tiles // per,)),
            dma, dma, dma, dma, dma((8,)),
        ],
        compiler_params=pltpu.CompilerParams(collective_id=0, has_side_effects=True, vmem_limit_bytes=LIMIT),
        name="em_step",
    )(genotypes, ancestry_counts.T, residuals.T, freqs)
    q_t, g_t, p_new, p_grad, z_flat = store(*results)
    return (q_t.T, g_t.T, p_new, p_grad, z_flat.reshape(anc, traits, mv))


def solution(mesh):
    in_specs = (
        P(("grp", "smp"), "var"),
        P(("grp", "smp"), None),
        P(("grp", "smp"), None),
        P("grp", "var"),
    )
    out_specs = (
        P(("grp", "smp", "var"), None),
        P(("grp", "smp", "var"), None),
        P("grp", "var"),
        P("grp", "var"),
        P("grp", None, "var"),
    )
    return jax.shard_map(shards, mesh=mesh, in_specs=in_specs, out_specs=out_specs, check_vma=False)
```

```python
import functools
import math

import jax
import jax.numpy as jnp
from jax import lax
from jax.experimental import pallas as pl
from jax.experimental.pallas import tpu as pltpu
from jax.sharding import PartitionSpec as P

MESH = pl.DeviceIdType.MESH
F32 = jnp.float32
BF16 = jnp.bfloat16
LIMIT = 67043328 - 491520
MOST = 5
NEAR_LAG = 3
LAG = 3


def normalize(fractions, gradient, second):
    weighted = fractions * (gradient + second[:, None])
    return weighted / jnp.sum(weighted, axis=1, keepdims=True)


def update_freqs(freqs, excess_sum, second_sum, sample_count):
    allele_sum = excess_sum + second_sum
    freq_next = freqs * allele_sum / (freqs * allele_sum + (1.0 - freqs) * second_sum)
    freq_gradient = excess_sum * freqs.shape[0] / math.sqrt(sample_count)
    return (freq_next, freq_gradient)


def shards_plain(genotypes, ancestry_counts, residuals, freqs):
    highest = lax.Precision.HIGHEST
    var_count = lax.axis_size("var")
    sample_rows = genotypes.shape[0]
    sample_count = sample_rows * lax.axis_size("smp")
    variant_count = genotypes.shape[1] * var_count
    anc_count = freqs.shape[0]
    trait_count = residuals.shape[1]
    counts = ancestry_counts.astype(jnp.float32)
    fractions = counts / jnp.sum(counts, axis=1, keepdims=True)
    dosage = genotypes.astype(jnp.float32)
    recon_rows = jnp.dot(fractions, freqs, precision=highest)
    ratio_a = dosage / recon_rows
    ratio_b = (2.0 - dosage) / (1.0 - recon_rows)
    excess = ratio_a - ratio_b
    gradient_part = jnp.dot(excess, freqs.T, precision=highest)
    second_part = jnp.sum(ratio_b, axis=1)
    excess_part = jnp.dot(fractions.T, excess, precision=highest)
    return_part = jnp.dot(fractions.T, ratio_b, precision=highest)
    share_rows = sample_rows // var_count
    first_row = lax.axis_index("var") * share_rows
    excess_sum, second_sum = lax.psum((excess_part, return_part), "smp")
    freq_next, freq_gradient = update_freqs(freqs, excess_sum, second_sum, sample_count)
    gradient_all, second_all = lax.psum((gradient_part, second_part), "var")
    fraction_next = normalize(fractions, gradient_all, second_all)
    own_next = lax.dynamic_slice_in_dim(fraction_next, first_row, share_rows, 0)
    own_gradient = lax.dynamic_slice_in_dim(gradient_all, first_row, share_rows, 0)
    scaled_gradient = own_gradient / math.sqrt(variant_count)
    ratio_next = dosage / jnp.dot(fraction_next, freqs, precision=highest)
    residual = residuals.astype(jnp.float32) / 1000.0
    trait_rows = (fraction_next[:, :, None] * residual[:, None, :]).reshape(
        sample_rows, anc_count * trait_count
    )
    score_part = jnp.dot(trait_rows.T, ratio_next, precision=highest)
    info_part = jnp.dot(
        (fraction_next * fraction_next).T, ratio_next * ratio_next, precision=highest
    )
    score_sum, info_sum = lax.psum((score_part, info_part), "smp")
    score_tiles = score_sum.reshape(anc_count, trait_count, genotypes.shape[1])
    z_score = score_tiles / jnp.sqrt(info_sum + 1e-06)[:, None, :]
    return (own_next, scaled_gradient, freq_next, freq_gradient, z_score)


def split(x):
    high = x.astype(BF16)
    return high, (x - high.astype(F32)).astype(BF16)


def dot(a, b):
    return jnp.dot(a, b, preferred_element_type=F32)


def dot_lanes(a, b):
    return lax.dot_general(a, b, (((1,), (1,)), ((), ())), preferred_element_type=F32)


def kernel(
    dims,
    geno_in, counts_in, resid_in, freqs_in,
    q_out, g_out, p_out, pg_out, z_out,
    geno, counts, resid, freqs, fstack, qf, gf, fcol, frow, ebuf, tbuf,
    acc_ex, acc_sc, acc_in,
    xs, xr, zs, er, mr, go, gp, fs, fr, ss, sr,
    xs_s, xs_r, z_s, z_r, m_s, m_r, xa_s, xa_r, f_s, f_r, s_s, s_r, in_s,
):
    chunks, width, half, parts, variant_count, sample_count, share, var_n = dims
    sub = width // 128
    anc = freqs.shape[0]
    traits = resid.shape[0]
    mv = freqs.shape[1]
    me = lax.axis_index("var")
    core = lax.axis_index("smp")
    x = lax.rem(me, 2)
    z = me // 2
    zn = z + 1 - 2 * lax.rem(z, 2)
    middle = jnp.logical_or(z == 1, z == 2)
    end = jnp.logical_or(z == 0, z == 3)
    partner = {"var": z * 2 + (1 - x)}
    twin = {"smp": 1 - core}
    beside = {"var": zn * 2 + x}
    across = {"var": lax.rem(7 - z, 4) * 2 + x}

    def load(src, dst, which, base=None, size=None):
        if base is not None:
            src, dst = src.at[pl.ds(base, size), :], dst.at[pl.ds(base, size), :]
        return pltpu.make_async_copy(src, dst, in_s.at[which])

    def load_lanes(src, dst, which, base, size):
        return pltpu.make_async_copy(
            src.at[:, pl.ds(base, size)], dst.at[:, pl.ds(base, size)], in_s.at[which]
        )

    far_half = pl.multiple_of((1 - x) * half, 128)
    near_half = pl.multiple_of(x * half, 128)
    freqs_load = load(freqs_in, freqs, 0)
    first_loads = (
        load_lanes(counts_in, counts, 1, far_half, width),
        load(geno_in, geno, 2, far_half, width),
    )
    later_loads = ()
    if chunks > 1:
        far_next = pl.multiple_of(far_half + width, 128)
        later_loads = (
            load_lanes(counts_in, counts, 3, far_next, half - width),
            load(geno_in, geno, 4, far_next, half - width),
        )
    near_loads = (
        load_lanes(counts_in, counts, 5, near_half, half),
        load(geno_in, geno, 6, near_half, half),
    )
    resid_load = load(resid_in, resid, 7)
    for item in (freqs_load,) + first_loads + later_loads + near_loads + (resid_load,):
        item.start()

    barrier = pltpu.get_barrier_semaphore()
    for peer in (partner, twin, beside):
        pl.semaphore_signal(barrier, inc=1, device_id=peer, device_id_type=MESH)

    @pl.when(middle)
    def _():
        pl.semaphore_signal(barrier, inc=1, device_id=across, device_id_type=MESH)

    acc_ex[...] = jnp.zeros_like(acc_ex)
    acc_sc[...] = jnp.zeros_like(acc_sc)
    acc_in[...] = jnp.zeros_like(acc_in)
    freqs_load.wait()
    p = freqs[...]
    p_hi, p_lo = split(p)
    stack = jnp.concatenate([p_hi.astype(F32), p_lo.astype(F32)] * 2, axis=0)
    fcol[...] = stack.T.astype(BF16)
    fstack[...] = stack.astype(BF16)
    frow[0:anc, 0:mv] = p_hi
    frow[0:anc, mv:] = p_hi
    frow[anc:, 0:mv] = p_lo
    frow[anc:, mv:] = p_lo

    def lanes(which, c):
        return pl.multiple_of(which * half + c * width, 128)

    def first_pass(off):
        d = geno[pl.ds(off, width), :].astype(F32).T
        c = counts[:, pl.ds(off, width)].astype(F32)
        total = jnp.sum(c, axis=0, keepdims=True)
        cb = c.astype(BF16)
        none = jnp.zeros_like(cb)
        u = dot(fcol[...], jnp.concatenate([cb, cb, none, none], axis=0))
        w = total - u
        inverse = 1.0 / (u * w)
        b = (2.0 - d) * u * inverse
        e = d * w * inverse - b
        e_hi, e_lo = split(e)
        b_hi, b_lo = split(b)
        ebuf[0:mv, :] = e_hi
        ebuf[mv : 2 * mv, :] = e_lo
        ebuf[2 * mv : 3 * mv, :] = b_hi
        ebuf[3 * mv :, :] = b_lo
        g = dot(frow[...], ebuf[0 : 2 * mv, :])
        acc_ex[...] += dot_lanes(ebuf[...], jnp.concatenate([cb] * (128 // anc), axis=0))
        return (g[0:anc, :] + g[anc:, :]) * total

    def second_pass(off, g):
        width = g.shape[1]
        c = counts[:, pl.ds(off, width)].astype(F32)
        f = c / jnp.sum(c, axis=0, keepdims=True)
        second = 2.0 * variant_count - jnp.sum(f * g, axis=0, keepdims=True)
        weighted = f * (g + second)
        q = weighted / jnp.sum(weighted, axis=0, keepdims=True)
        qf[:, pl.ds(off, width)] = q
        gf[:, pl.ds(off, width)] = g * (1.0 / math.sqrt(variant_count))
        q_hi, q_lo = split(q)
        recon = lax.dot_general(
            jnp.concatenate([q_hi, q_hi, q_lo, q_lo], axis=0),
            fstack[...],
            (((0,), (0,)), ((), ())),
            preferred_element_type=F32,
        )
        r = geno[pl.ds(off, width), :].astype(F32) / recon
        r_hi, r_lo = split(r)
        s_hi, s_lo = split(r * r)
        t = resid[:, pl.ds(off, width)].astype(F32)
        r_cat = jnp.concatenate([r_hi, r_lo], axis=1)
        r_cat = jnp.concatenate([r_cat, r_cat], axis=0)
        step = anc // 2
        for m in range(2):
            for k in range(step * m, step * (m + 1)):
                t_hi, t_lo = split(q[k : k + 1, :] * t)
                tbuf[traits * k : traits * (k + 1), 0:width] = t_hi
                tbuf[traits * k : traits * (k + 1), width : 2 * width] = t_lo
            at = slice(traits * step * m, traits * step * (m + 1))
            o = dot(tbuf[at, 0 : 2 * width], r_cat)
            acc_sc[at, :] += o[:, 0:mv] + o[:, mv:]
        y_hi, y_lo = split(q * q)
        none = jnp.zeros_like(y_hi)
        acc_in[...] += dot(
            jnp.concatenate([y_hi, y_lo], axis=0), jnp.concatenate([s_hi, s_lo], axis=1)
        )

    def copy(src, dst, send, recv, peer):
        return pltpu.make_async_remote_copy(
            src_ref=src, dst_ref=dst, send_sem=send, recv_sem=recv, device_id=peer, device_id_type=MESH
        )

    def x_reduce(t):
        return copy(xs.at[t], xr.at[t], xs_s, xs_r.at[t], partner)

    def inward(t):
        return copy(zs.at[t], er.at[t], z_s, z_r.at[t], beside)

    def exchange(t):
        return copy(zs.at[t], mr.at[t], m_s, m_r.at[t], across)

    def outward(t):
        return copy(go.at[t], go.at[t], z_s, z_r.at[t], beside)

    def part_of(t):
        return sum(jnp.int32(t >= at) for at, _ in parts[1:])

    def x_gather(t):
        return copy(go.at[t], gp.at[t], xa_s, xa_r.at[part_of(t)], partner)

    def x_gathered(n):
        at = pl.ds(*parts[n])
        return copy(go.at[at], gp.at[at], xa_s, xa_r.at[n], partner)

    def put(ref, c, g):
        for j in range(sub):
            ref[c * sub + j] = g[:, 128 * j : 128 * (j + 1)]

    def take(ref, at, count):
        return jnp.concatenate([ref[at + j] for j in range(count)], axis=1)

    for item in first_loads:
        item.wait()
    put(xs, 0, first_pass(lanes(1 - x, 0)))

    @pl.when(middle)
    def _():
        pl.semaphore_wait(barrier, 4)

    @pl.when(end)
    def _():
        pl.semaphore_wait(barrier, 3)

    for j in range(sub):
        x_reduce(j).start()
    for item in later_loads:
        item.wait()

    def step_far(c, carry):
        put(xs, c, first_pass(lanes(1 - x, c)))
        for j in range(sub):
            x_reduce(c * sub + j).start()
        return carry

    lax.fori_loop(1, chunks, step_far, 0)
    for item in near_loads:
        item.wait()

    def add_inward(t):
        inward(t).wait_recv()
        zs[t] = zs[t] + er[t]
        exchange(t).start()

    def add_exchange(c, j):
        t = c * sub + j
        exchange(t).wait_recv()
        go[t] = zs[t] + mr[t]
        outward(t).start()
        x_gather(t).start()

    def step_near(c, carry):
        put(zs, c, first_pass(lanes(x, c)))
        for j in range(sub):
            t = c * sub + j
            x_reduce(t).wait_recv()
            zs[t] = zs[t] + xr[t]

            @pl.when(end)
            def _(t=t):
                inward(t).start()

            @pl.when(jnp.logical_and(middle, c >= NEAR_LAG))
            def _(t=t):
                add_inward(t - NEAR_LAG * sub)

        return carry

    lax.fori_loop(0, chunks, step_near, 0)

    ex = acc_ex[0:mv, :] + acc_ex[mv : 2 * mv, :]
    re = acc_ex[2 * mv : 3 * mv, :] + acc_ex[3 * mv :, :]
    fs[0:anc, :] = ex.T[0:anc, :]
    fs[anc:, :] = re.T[0:anc, :]
    freq_copy = copy(fs, fr, f_s, f_r, twin)
    freq_copy.start()

    @pl.when(middle)
    def _():
        def step_inward(t, carry):
            add_inward(t)
            return carry

        def step_exchange(c, carry):
            for j in range(sub):
                t = c * sub + j

                @pl.when(c + LAG < chunks)
                def _(t=t):
                    add_inward(t + LAG * sub)

                add_exchange(c, j)
            return carry

        for t in range(max(0, chunks - NEAR_LAG) * sub, min(LAG, chunks) * sub):
            step_inward(t, 0)
        for c in range(chunks):
            step_exchange(c, 0)

    resid_load.wait()

    def step_own(c, carry):
        for j in range(sub):
            t = c * sub + j

            @pl.when(end)
            def _(t=t):
                outward(t).wait_recv()
                x_gather(t).start()

        second_pass(pl.multiple_of(x * half + c * sub * 128, 128), take(go, c * sub, sub))
        return carry

    lax.fori_loop(0, chunks * sub // sub, step_own, 0)

    for n, (at, count) in enumerate(parts):
        x_gathered(n).wait_recv()
        second_pass(pl.multiple_of((1 - x) * half + at * 128, 128), take(gp, at, count))

    tiles = anc * traits
    ss[0:tiles, :] = acc_sc[...]
    info = acc_in[0:anc, :] + acc_in[anc:, :]
    ss[tiles:, :] = info[:, 0:mv] + info[:, mv:]
    score_copy = copy(ss, sr, s_s, s_r, twin)
    score_copy.start()

    freq_copy.wait_recv()
    sums = fs[...] + fr[...]
    excess_sum = sums[0:anc, :]
    second_sum = sums[anc:, :]
    freq_next, freq_gradient = update_freqs(freqs[...], excess_sum, second_sum, sample_count)
    p_out[...] = freq_next
    pg_out[...] = freq_gradient

    for v in range(var_n):

        @pl.when(me == v)
        def _():
            q_out[...] = qf[:, share * v : share * (v + 1)]
            g_out[...] = gf[:, share * v : share * (v + 1)]

    copy(xs, xr, xs_s, xs_r.at[0], partner).wait_send()
    copy(go, gp, xa_s, xa_r.at[0], partner).wait_send()
    copy(zs, er, z_s, z_r.at[0], beside).wait_send()

    @pl.when(middle)
    def _():
        copy(zs, mr, m_s, m_r.at[0], across).wait_send()

    freq_copy.wait_send()
    score_copy.wait_recv()
    info_sum = ss[tiles:, :] + sr[tiles:, :]
    scale = 0.001 / jnp.sqrt(info_sum + 1e-06)
    for k in range(anc):
        at = slice(traits * k, traits * (k + 1))
        z_out[at, :] = (ss[at, :] + sr[at, :]) * scale[k : k + 1, :]
    score_copy.wait_send()


def store_kernel(*refs):
    count = len(refs) // 2
    sems = refs[-1]
    copies = [pltpu.make_async_copy(refs[i], refs[count + i], sems.at[i]) for i in range(count)]
    for item in copies:
        item.start()
    for item in copies:
        item.wait()


def store(*arrays):
    return pl.pallas_call(
        store_kernel,
        out_shape=tuple(jax.ShapeDtypeStruct(a.shape, a.dtype) for a in arrays),
        in_specs=[pl.BlockSpec(memory_space=pltpu.VMEM)] * len(arrays),
        out_specs=(pl.BlockSpec(memory_space=pl.ANY),) * len(arrays),
        scratch_shapes=[pltpu.SemaphoreType.DMA((len(arrays),))],
        compiler_params=pltpu.CompilerParams(vmem_limit_bytes=1024 * 1024),
        name="store",
    )(*arrays)


def split_tiles(tiles):
    sizes = [MOST] * max(0, (tiles - 1) // MOST)
    rest = tiles - sum(sizes)
    sizes += [size for size in (rest - rest // 2, rest // 2) if size]
    starts = [sum(sizes[:i]) for i in range(len(sizes))]
    return tuple(zip(starts, sizes))


def fits(genotypes, residuals, freqs, var_n):
    samples, mv = genotypes.shape
    anc = freqs.shape[0]
    return (
        var_n == 8
        and lax.axis_size("smp") == 2
        and anc == 32
        and mv == 128
        and residuals.shape[1] % 16 == 0
        and samples % (2 * 128) == 0
        and samples % var_n == 0
    )


def shards(genotypes, ancestry_counts, residuals, freqs):
    var_n = lax.axis_size("var")
    if not fits(genotypes, residuals, freqs, var_n):
        return shards_plain(genotypes, ancestry_counts, residuals, freqs)
    samples, mv = genotypes.shape
    anc = freqs.shape[0]
    traits = residuals.shape[1]
    half = samples // 2
    tiles = half // 128
    chunks = max(n for n in range(1, MOST + 1) if tiles % n == 0)
    width = half // chunks
    parts = split_tiles(tiles)
    share = samples // var_n
    dims = (chunks, width, half, parts, mv * var_n, samples * lax.axis_size("smp"), share, var_n)
    vmem = pl.BlockSpec(memory_space=pltpu.VMEM)
    dma = pltpu.SemaphoreType.DMA
    part = pltpu.VMEM((half // 128, anc, 128), F32)
    flags = dma((half // 128,))
    results = pl.pallas_call(
        functools.partial(kernel, dims),
        out_shape=(
            pltpu.VMEM((anc, share), F32),
            pltpu.VMEM((anc, share), F32),
            pltpu.VMEM((anc, mv), F32),
            pltpu.VMEM((anc, mv), F32),
            pltpu.VMEM((anc * traits, mv), F32),
        ),
        in_specs=[pl.BlockSpec(memory_space=pltpu.HBM)] * 4,
        out_specs=(vmem,) * 5,
        scratch_shapes=[
            pltpu.VMEM((samples, mv), BF16),
            pltpu.VMEM((anc, samples), jnp.int32),
            pltpu.VMEM((traits, samples), jnp.int32),
            pltpu.VMEM((anc, mv), F32),
            pltpu.VMEM((4 * anc, mv), BF16),
            pltpu.VMEM((anc, samples), F32),
            pltpu.VMEM((anc, samples), F32),
            pltpu.VMEM((mv, 4 * anc), BF16),
            pltpu.VMEM((2 * anc, 2 * mv), BF16),
            pltpu.VMEM((4 * mv, width), BF16),
            pltpu.VMEM((anc * traits, 256 * max(width // 128, MOST)), BF16),
            pltpu.VMEM((4 * mv, 128), F32),
            pltpu.VMEM((anc * traits, mv), F32),
            pltpu.VMEM((2 * anc, 2 * mv), F32),
            part, part, part, part, part, part, part,
            pltpu.VMEM((2 * anc, mv), F32),
            pltpu.VMEM((2 * anc, mv), F32),
            pltpu.VMEM((anc * traits + anc, mv), F32),
            pltpu.VMEM((anc * traits + anc, mv), F32),
            dma, flags, dma, flags, dma, flags, dma, dma((len(parts),)),
            dma, dma, dma, dma, dma((8,)),
        ],
        compiler_params=pltpu.CompilerParams(collective_id=0, has_side_effects=True, vmem_limit_bytes=LIMIT),
        name="em_step",
    )(genotypes, ancestry_counts.T, residuals.T, freqs)
    q_t, g_t, p_new, p_grad, z_flat = store(*results)
    return (q_t.T, g_t.T, p_new, p_grad, z_flat.reshape(anc, traits, mv))


def solution(mesh):
    in_specs = (
        P(("grp", "smp"), "var"),
        P(("grp", "smp"), None),
        P(("grp", "smp"), None),
        P("grp", "var"),
    )
    out_specs = (
        P(("grp", "smp", "var"), None),
        P(("grp", "smp", "var"), None),
        P("grp", "var"),
        P("grp", "var"),
        P("grp", None, "var"),
    )
    return jax.shard_map(shards, mesh=mesh, in_specs=in_specs, out_specs=out_specs, check_vma=False)
```

```python
import functools
import math

import jax
import jax.numpy as jnp
from jax import lax
from jax.experimental import pallas as pl
from jax.experimental.pallas import tpu as pltpu
from jax.sharding import PartitionSpec as P

MESH = pl.DeviceIdType.MESH
F32 = jnp.float32
BF16 = jnp.bfloat16
LIMIT = 67043328 - 491520
MOST = 5
NEAR_LAG = 2
OWN = 3
OTHER = 5
LAG = 3


def normalize(fractions, gradient, second):
    weighted = fractions * (gradient + second[:, None])
    return weighted / jnp.sum(weighted, axis=1, keepdims=True)


def update_freqs(freqs, excess_sum, second_sum, sample_count):
    allele_sum = excess_sum + second_sum
    freq_next = freqs * allele_sum / (freqs * allele_sum + (1.0 - freqs) * second_sum)
    freq_gradient = excess_sum * freqs.shape[0] / math.sqrt(sample_count)
    return (freq_next, freq_gradient)


def shards_plain(genotypes, ancestry_counts, residuals, freqs):
    highest = lax.Precision.HIGHEST
    var_count = lax.axis_size("var")
    sample_rows = genotypes.shape[0]
    sample_count = sample_rows * lax.axis_size("smp")
    variant_count = genotypes.shape[1] * var_count
    anc_count = freqs.shape[0]
    trait_count = residuals.shape[1]
    counts = ancestry_counts.astype(jnp.float32)
    fractions = counts / jnp.sum(counts, axis=1, keepdims=True)
    dosage = genotypes.astype(jnp.float32)
    recon_rows = jnp.dot(fractions, freqs, precision=highest)
    ratio_a = dosage / recon_rows
    ratio_b = (2.0 - dosage) / (1.0 - recon_rows)
    excess = ratio_a - ratio_b
    gradient_part = jnp.dot(excess, freqs.T, precision=highest)
    second_part = jnp.sum(ratio_b, axis=1)
    excess_part = jnp.dot(fractions.T, excess, precision=highest)
    return_part = jnp.dot(fractions.T, ratio_b, precision=highest)
    share_rows = sample_rows // var_count
    first_row = lax.axis_index("var") * share_rows
    excess_sum, second_sum = lax.psum((excess_part, return_part), "smp")
    freq_next, freq_gradient = update_freqs(freqs, excess_sum, second_sum, sample_count)
    gradient_all, second_all = lax.psum((gradient_part, second_part), "var")
    fraction_next = normalize(fractions, gradient_all, second_all)
    own_next = lax.dynamic_slice_in_dim(fraction_next, first_row, share_rows, 0)
    own_gradient = lax.dynamic_slice_in_dim(gradient_all, first_row, share_rows, 0)
    scaled_gradient = own_gradient / math.sqrt(variant_count)
    ratio_next = dosage / jnp.dot(fraction_next, freqs, precision=highest)
    residual = residuals.astype(jnp.float32) / 1000.0
    trait_rows = (fraction_next[:, :, None] * residual[:, None, :]).reshape(
        sample_rows, anc_count * trait_count
    )
    score_part = jnp.dot(trait_rows.T, ratio_next, precision=highest)
    info_part = jnp.dot(
        (fraction_next * fraction_next).T, ratio_next * ratio_next, precision=highest
    )
    score_sum, info_sum = lax.psum((score_part, info_part), "smp")
    score_tiles = score_sum.reshape(anc_count, trait_count, genotypes.shape[1])
    z_score = score_tiles / jnp.sqrt(info_sum + 1e-06)[:, None, :]
    return (own_next, scaled_gradient, freq_next, freq_gradient, z_score)


def split(x):
    high = x.astype(BF16)
    return high, (x - high.astype(F32)).astype(BF16)


def dot(a, b):
    return jnp.dot(a, b, preferred_element_type=F32)


def dot_lanes(a, b):
    return lax.dot_general(a, b, (((1,), (1,)), ((), ())), preferred_element_type=F32)


def kernel(
    dims,
    geno_in, counts_in, resid_in, freqs_in,
    q_out, g_out, p_out, pg_out, z_out,
    geno, counts, resid, freqs, fstack, qf, gf, fcol, frow, ebuf, tbuf,
    acc_ex, acc_sc, acc_in,
    xs, xr, zs, er, mr, go, gp, fs, fr, ss, sr,
    xs_s, xs_r, z_s, z_r, m_s, m_r, xa_s, xa_r, f_s, f_r, s_s, s_r, in_s,
):
    chunks, width, half, own_per, per, variant_count, sample_count, share, var_n = dims
    sub = width // 128
    anc = freqs.shape[0]
    traits = resid.shape[0]
    mv = freqs.shape[1]
    me = lax.axis_index("var")
    core = lax.axis_index("smp")
    x = lax.rem(me, 2)
    z = me // 2
    zn = z + 1 - 2 * lax.rem(z, 2)
    middle = jnp.logical_or(z == 1, z == 2)
    end = jnp.logical_or(z == 0, z == 3)
    partner = {"var": z * 2 + (1 - x)}
    twin = {"smp": 1 - core}
    beside = {"var": zn * 2 + x}
    across = {"var": lax.rem(7 - z, 4) * 2 + x}

    def load(src, dst, which, base=None, size=None):
        if base is not None:
            src, dst = src.at[pl.ds(base, size), :], dst.at[pl.ds(base, size), :]
        return pltpu.make_async_copy(src, dst, in_s.at[which])

    def load_lanes(src, dst, which, base, size):
        return pltpu.make_async_copy(
            src.at[:, pl.ds(base, size)], dst.at[:, pl.ds(base, size)], in_s.at[which]
        )

    far_half = pl.multiple_of((1 - x) * half, 128)
    near_half = pl.multiple_of(x * half, 128)
    freqs_load = load(freqs_in, freqs, 0)
    first_loads = (
        load_lanes(counts_in, counts, 1, far_half, width),
        load(geno_in, geno, 2, far_half, width),
    )
    later_loads = ()
    if chunks > 1:
        far_next = pl.multiple_of(far_half + width, 128)
        later_loads = (
            load_lanes(counts_in, counts, 3, far_next, half - width),
            load(geno_in, geno, 4, far_next, half - width),
        )
    near_loads = (
        load_lanes(counts_in, counts, 5, near_half, half),
        load(geno_in, geno, 6, near_half, half),
    )
    resid_load = load(resid_in, resid, 7)
    for item in (freqs_load,) + first_loads + later_loads + near_loads + (resid_load,):
        item.start()

    barrier = pltpu.get_barrier_semaphore()
    for peer in (partner, twin, beside):
        pl.semaphore_signal(barrier, inc=1, device_id=peer, device_id_type=MESH)

    @pl.when(middle)
    def _():
        pl.semaphore_signal(barrier, inc=1, device_id=across, device_id_type=MESH)

    acc_ex[...] = jnp.zeros_like(acc_ex)
    acc_sc[...] = jnp.zeros_like(acc_sc)
    acc_in[...] = jnp.zeros_like(acc_in)
    freqs_load.wait()
    p = freqs[...]
    p_hi, p_lo = split(p)
    stack = jnp.concatenate([p_hi.astype(F32), p_lo.astype(F32)] * 2, axis=0)
    fcol[...] = stack.T.astype(BF16)
    fstack[...] = stack.astype(BF16)
    frow[0:anc, 0:mv] = p_hi
    frow[0:anc, mv:] = p_hi
    frow[anc:, 0:mv] = p_lo
    frow[anc:, mv:] = p_lo

    def lanes(which, c):
        return pl.multiple_of(which * half + c * width, 128)

    def first_pass(off):
        d = geno[pl.ds(off, width), :].astype(F32).T
        c = counts[:, pl.ds(off, width)].astype(F32)
        total = jnp.sum(c, axis=0, keepdims=True)
        cb = c.astype(BF16)
        none = jnp.zeros_like(cb)
        u = dot(fcol[...], jnp.concatenate([cb, cb, none, none], axis=0))
        w = total - u
        inverse = 1.0 / (u * w)
        b = (2.0 - d) * u * inverse
        e = d * w * inverse - b
        e_hi, e_lo = split(e)
        b_hi, b_lo = split(b)
        ebuf[0:mv, :] = e_hi
        ebuf[mv : 2 * mv, :] = e_lo
        ebuf[2 * mv : 3 * mv, :] = b_hi
        ebuf[3 * mv :, :] = b_lo
        g = dot(frow[...], ebuf[0 : 2 * mv, :])
        acc_ex[...] += dot_lanes(ebuf[...], jnp.concatenate([cb] * (128 // anc), axis=0))
        return (g[0:anc, :] + g[anc:, :]) * total

    def second_pass(off, g):
        width = g.shape[1]
        c = counts[:, pl.ds(off, width)].astype(F32)
        f = c / jnp.sum(c, axis=0, keepdims=True)
        second = 2.0 * variant_count - jnp.sum(f * g, axis=0, keepdims=True)
        weighted = f * (g + second)
        q = weighted / jnp.sum(weighted, axis=0, keepdims=True)
        qf[:, pl.ds(off, width)] = q
        gf[:, pl.ds(off, width)] = g * (1.0 / math.sqrt(variant_count))
        q_hi, q_lo = split(q)
        recon = lax.dot_general(
            jnp.concatenate([q_hi, q_hi, q_lo, q_lo], axis=0),
            fstack[...],
            (((0,), (0,)), ((), ())),
            preferred_element_type=F32,
        )
        r = geno[pl.ds(off, width), :].astype(F32) / recon
        r_hi, r_lo = split(r)
        s_hi, s_lo = split(r * r)
        t = resid[:, pl.ds(off, width)].astype(F32)
        r_cat = jnp.concatenate([r_hi, r_lo], axis=1)
        r_cat = jnp.concatenate([r_cat, r_cat], axis=0)
        step = anc // 2
        for m in range(2):
            for k in range(step * m, step * (m + 1)):
                t_hi, t_lo = split(q[k : k + 1, :] * t)
                tbuf[traits * k : traits * (k + 1), 0:width] = t_hi
                tbuf[traits * k : traits * (k + 1), width : 2 * width] = t_lo
            at = slice(traits * step * m, traits * step * (m + 1))
            o = dot(tbuf[at, 0 : 2 * width], r_cat)
            acc_sc[at, :] += o[:, 0:mv] + o[:, mv:]
        y_hi, y_lo = split(q * q)
        none = jnp.zeros_like(y_hi)
        acc_in[...] += dot(
            jnp.concatenate([y_hi, y_lo], axis=0), jnp.concatenate([s_hi, s_lo], axis=1)
        )

    def copy(src, dst, send, recv, peer):
        return pltpu.make_async_remote_copy(
            src_ref=src, dst_ref=dst, send_sem=send, recv_sem=recv, device_id=peer, device_id_type=MESH
        )

    def x_reduce(t):
        return copy(xs.at[t], xr.at[t], xs_s, xs_r.at[t], partner)

    def inward(t):
        return copy(zs.at[t], er.at[t], z_s, z_r.at[t], beside)

    def exchange(t):
        return copy(zs.at[t], mr.at[t], m_s, m_r.at[t], across)

    def outward(t):
        return copy(go.at[t], go.at[t], z_s, z_r.at[t], beside)

    def x_gather(t):
        return copy(go.at[t], gp.at[t], xa_s, xa_r.at[t // per], partner)

    def x_gathered(c):
        at = pl.ds(c * per, per)
        return copy(go.at[at], gp.at[at], xa_s, xa_r.at[c], partner)

    def put(ref, c, g):
        for j in range(sub):
            ref[c * sub + j] = g[:, 128 * j : 128 * (j + 1)]

    def take(ref, at, count):
        return jnp.concatenate([ref[at + j] for j in range(count)], axis=1)

    for item in first_loads:
        item.wait()
    put(xs, 0, first_pass(lanes(1 - x, 0)))

    @pl.when(middle)
    def _():
        pl.semaphore_wait(barrier, 4)

    @pl.when(end)
    def _():
        pl.semaphore_wait(barrier, 3)

    for j in range(sub):
        x_reduce(j).start()
    for item in later_loads:
        item.wait()

    def step_far(c, carry):
        put(xs, c, first_pass(lanes(1 - x, c)))
        for j in range(sub):
            x_reduce(c * sub + j).start()
        return carry

    lax.fori_loop(1, chunks, step_far, 0)
    for item in near_loads:
        item.wait()

    def add_inward(t):
        inward(t).wait_recv()
        zs[t] = zs[t] + er[t]
        exchange(t).start()

    def add_exchange(c, j):
        t = c * sub + j
        exchange(t).wait_recv()
        go[t] = zs[t] + mr[t]
        outward(t).start()
        x_gather(t).start()

    def step_near(c, carry):
        put(zs, c, first_pass(lanes(x, c)))
        for j in range(sub):
            t = c * sub + j
            x_reduce(t).wait_recv()
            zs[t] = zs[t] + xr[t]

            @pl.when(end)
            def _(t=t):
                inward(t).start()

            @pl.when(jnp.logical_and(middle, c >= NEAR_LAG))
            def _(t=t):
                add_inward(t - NEAR_LAG * sub)

        return carry

    lax.fori_loop(0, chunks, step_near, 0)

    ex = acc_ex[0:mv, :] + acc_ex[mv : 2 * mv, :]
    re = acc_ex[2 * mv : 3 * mv, :] + acc_ex[3 * mv :, :]
    fs[0:anc, :] = ex.T[0:anc, :]
    fs[anc:, :] = re.T[0:anc, :]
    freq_copy = copy(fs, fr, f_s, f_r, twin)
    freq_copy.start()

    @pl.when(middle)
    def _():
        def step_inward(t, carry):
            add_inward(t)
            return carry

        def step_exchange(c, carry):
            for j in range(sub):
                t = c * sub + j

                @pl.when(c + LAG < chunks)
                def _(t=t):
                    add_inward(t + LAG * sub)

                add_exchange(c, j)
            return carry

        lax.fori_loop(max(0, chunks - NEAR_LAG) * sub, min(LAG, chunks) * sub, step_inward, 0)
        lax.fori_loop(0, chunks, step_exchange, 0)

    resid_load.wait()

    def step_own(c, carry):
        for j in range(own_per):
            t = c * own_per + j

            @pl.when(end)
            def _(t=t):
                outward(t).wait_recv()
                x_gather(t).start()

        second_pass(pl.multiple_of(x * half + c * own_per * 128, 128), take(go, c * own_per, own_per))
        return carry

    lax.fori_loop(0, chunks * sub // own_per, step_own, 0)

    def step_other(c, carry):
        x_gathered(c).wait_recv()
        second_pass(pl.multiple_of((1 - x) * half + c * per * 128, 128), take(gp, c * per, per))
        return carry

    lax.fori_loop(0, chunks * sub // per, step_other, 0)

    tiles = anc * traits
    ss[0:tiles, :] = acc_sc[...]
    info = acc_in[0:anc, :] + acc_in[anc:, :]
    ss[tiles:, :] = info[:, 0:mv] + info[:, mv:]
    score_copy = copy(ss, sr, s_s, s_r, twin)
    score_copy.start()

    freq_copy.wait_recv()
    sums = fs[...] + fr[...]
    excess_sum = sums[0:anc, :]
    second_sum = sums[anc:, :]
    freq_next, freq_gradient = update_freqs(freqs[...], excess_sum, second_sum, sample_count)
    p_out[...] = freq_next
    pg_out[...] = freq_gradient

    for v in range(var_n):

        @pl.when(me == v)
        def _():
            q_out[...] = qf[:, share * v : share * (v + 1)]
            g_out[...] = gf[:, share * v : share * (v + 1)]

    copy(xs, xr, xs_s, xs_r.at[0], partner).wait_send()
    copy(go, gp, xa_s, xa_r.at[0], partner).wait_send()
    copy(zs, er, z_s, z_r.at[0], beside).wait_send()

    @pl.when(middle)
    def _():
        copy(zs, mr, m_s, m_r.at[0], across).wait_send()

    freq_copy.wait_send()
    score_copy.wait_recv()
    info_sum = ss[tiles:, :] + sr[tiles:, :]
    scale = 0.001 / jnp.sqrt(info_sum + 1e-06)
    for k in range(anc):
        at = slice(traits * k, traits * (k + 1))
        z_out[at, :] = (ss[at, :] + sr[at, :]) * scale[k : k + 1, :]
    score_copy.wait_send()


def store_kernel(*refs):
    count = len(refs) // 2
    sems = refs[-1]
    copies = [pltpu.make_async_copy(refs[i], refs[count + i], sems.at[i]) for i in range(count)]
    for item in copies:
        item.start()
    for item in copies:
        item.wait()


def store(*arrays):
    return pl.pallas_call(
        store_kernel,
        out_shape=tuple(jax.ShapeDtypeStruct(a.shape, a.dtype) for a in arrays),
        in_specs=[pl.BlockSpec(memory_space=pltpu.VMEM)] * len(arrays),
        out_specs=(pl.BlockSpec(memory_space=pl.ANY),) * len(arrays),
        scratch_shapes=[pltpu.SemaphoreType.DMA((len(arrays),))],
        compiler_params=pltpu.CompilerParams(vmem_limit_bytes=1024 * 1024),
        name="store",
    )(*arrays)


def fits(genotypes, residuals, freqs, var_n):
    samples, mv = genotypes.shape
    anc = freqs.shape[0]
    return (
        var_n == 8
        and lax.axis_size("smp") == 2
        and anc == 32
        and mv == 128
        and residuals.shape[1] % 16 == 0
        and samples % (2 * 128) == 0
        and samples % var_n == 0
    )


def shards(genotypes, ancestry_counts, residuals, freqs):
    var_n = lax.axis_size("var")
    if not fits(genotypes, residuals, freqs, var_n):
        return shards_plain(genotypes, ancestry_counts, residuals, freqs)
    samples, mv = genotypes.shape
    anc = freqs.shape[0]
    traits = residuals.shape[1]
    half = samples // 2
    tiles = half // 128
    chunks = max(n for n in range(1, MOST + 1) if tiles % n == 0)
    width = half // chunks
    own_per = max(n for n in range(1, OWN + 1) if tiles % n == 0)
    per = max(n for n in range(1, OTHER + 1) if tiles % n == 0)
    share = samples // var_n
    dims = (chunks, width, half, own_per, per, mv * var_n, samples * lax.axis_size("smp"), share, var_n)
    vmem = pl.BlockSpec(memory_space=pltpu.VMEM)
    dma = pltpu.SemaphoreType.DMA
    part = pltpu.VMEM((half // 128, anc, 128), F32)
    flags = dma((half // 128,))
    results = pl.pallas_call(
        functools.partial(kernel, dims),
        out_shape=(
            pltpu.VMEM((anc, share), F32),
            pltpu.VMEM((anc, share), F32),
            pltpu.VMEM((anc, mv), F32),
            pltpu.VMEM((anc, mv), F32),
            pltpu.VMEM((anc * traits, mv), F32),
        ),
        in_specs=[pl.BlockSpec(memory_space=pltpu.HBM)] * 4,
        out_specs=(vmem,) * 5,
        scratch_shapes=[
            pltpu.VMEM((samples, mv), BF16),
            pltpu.VMEM((anc, samples), jnp.int32),
            pltpu.VMEM((traits, samples), jnp.int32),
            pltpu.VMEM((anc, mv), F32),
            pltpu.VMEM((4 * anc, mv), BF16),
            pltpu.VMEM((anc, samples), F32),
            pltpu.VMEM((anc, samples), F32),
            pltpu.VMEM((mv, 4 * anc), BF16),
            pltpu.VMEM((2 * anc, 2 * mv), BF16),
            pltpu.VMEM((4 * mv, width), BF16),
            pltpu.VMEM((anc * traits, 256 * max(own_per, per)), BF16),
            pltpu.VMEM((4 * mv, 128), F32),
            pltpu.VMEM((anc * traits, mv), F32),
            pltpu.VMEM((2 * anc, 2 * mv), F32),
            part, part, part, part, part, part, part,
            pltpu.VMEM((2 * anc, mv), F32),
            pltpu.VMEM((2 * anc, mv), F32),
            pltpu.VMEM((anc * traits + anc, mv), F32),
            pltpu.VMEM((anc * traits + anc, mv), F32),
            dma, flags, dma, flags, dma, flags, dma, dma((tiles // per,)),
            dma, dma, dma, dma, dma((8,)),
        ],
        compiler_params=pltpu.CompilerParams(collective_id=0, has_side_effects=True, vmem_limit_bytes=LIMIT),
        name="em_step",
    )(genotypes, ancestry_counts.T, residuals.T, freqs)
    q_t, g_t, p_new, p_grad, z_flat = store(*results)
    return (q_t.T, g_t.T, p_new, p_grad, z_flat.reshape(anc, traits, mv))


def solution(mesh):
    in_specs = (
        P(("grp", "smp"), "var"),
        P(("grp", "smp"), None),
        P(("grp", "smp"), None),
        P("grp", "var"),
    )
    out_specs = (
        P(("grp", "smp", "var"), None),
        P(("grp", "smp", "var"), None),
        P("grp", "var"),
        P("grp", "var"),
        P("grp", None, "var"),
    )
    return jax.shard_map(shards, mesh=mesh, in_specs=in_specs, out_specs=out_specs, check_vma=False)
```
